256 devices in a mesh: grp: 2 (over z), row: 128 (over y, x, core).
Axes of the slice: x: 8, y: 8, z: 2, core: 2. Of those that a mesh axis runs over, the one named last changes fastest.
The devices are a block of a 8x8x16 slice.
Arguments:
- source_emb: bfloat16 [1048576, 256], P(('grp', 'row')), parts along dimension 0, may hold values from -6 to 6
- target_emb: bfloat16 [1048576, 256], P(('grp', 'row')), parts along dimension 0, may hold values from -6 to 6
- source_cluster: int32 [1048576], P(('grp', 'row')), parts along dimension 0, may hold values from 0 to 4095, never falling along the last dimension, each value on 1 to 256 neighbouring positions
- target_cluster: int32 [1048576], P(('grp', 'row')), parts along dimension 0, may hold values from 0 to 4095, never falling along the last dimension, each value on 1 to 256 neighbouring positions
- coarse_source: float32 [8192], P('grp'), parts along dimension 0, may hold values from -3 to 3
- coarse_target: float32 [8192], P('grp'), parts along dimension 0, may hold values from -3 to 3
- block_list: int32 [8192, 8], P(('grp', 'row')), parts along dimension 0, may hold values from 0 to 4095, as said below
- block_count: int32 [8192], P(('grp', 'row')), parts along dimension 0, may hold values from 1 to 8, as said below
Outputs:
- source_potential: float32 [1048576], P(('grp', 'row')), parts along dimension 0
- target_potential: float32 [1048576], P(('grp', 'row')), parts along dimension 0
The draws below stay inside these ranges and needn't reach their ends.
There are 2 independent parts, one for each index of `grp`. The reference program is written for one: setup_inputs(seed, part) draws one part's arguments, and reference() takes and returns one part's arrays. A program takes and returns all parts, laid end to end along the dimension named above; each array names one. Nothing has to cross between parts.
Inputs may be any that keep to these rules, and one draw needn't show every extreme that they name: Each row of block_list names 8 different target tiles, each within 1 device of the source tile's device (tile index divided by 32); entry 0 is the target tile with the source tile's own index. Only the first block_count entries of a row are active. `block_count`: some source tile has 8 active entries in every draw.
All inputs are finite; a program needn't handle non-finite values.
Results may differ from the reference program's by a relative error of at most 0.0003.
Values may be sent and summed in bfloat16 or wider, within the bound.
A program may use at most 64 MiB of HBM per device.

```python
import math
import jax
import jax.numpy as jnp
import numpy as np
from jax import lax

EMBED = 256
CLUSTERS = 4096
TILE = 128
REACH = 1
MAXB = 8
ITERS = 2
TILES_DEV = 32
SOURCES = 524288
TARGETS = 524288
TILE_COUNT = 4096


def embedding_pair(key):
    base = jax.random.fold_in(key, 7)
    keys = jax.random.split(base, 2)
    shape = (SOURCES, EMBED)
    source = jnp.clip(jax.random.normal(keys[0], shape) * 0.25, -1.5, 1.5)
    target = jnp.clip(jax.random.normal(keys[1], shape) * 0.25, -1.5, 1.5)
    return (source, target)


def draw_source_emb(key, part):
    return embedding_pair(key)[0].astype(jnp.bfloat16)


def draw_target_emb(key, part):
    return embedding_pair(key)[1].astype(jnp.bfloat16)


def draw_block_list(key, part):
    stream = jax.random.fold_in(key, 31)
    span_tiles = (2 * REACH + 1) * TILES_DEV
    device_of = jnp.arange(TILE_COUNT, dtype=jnp.int32) // TILES_DEV
    position = jnp.arange(span_tiles, dtype=jnp.int32)
    candidate = (device_of[:, None] - REACH) * TILES_DEV + position[None, :]
    inside = (candidate >= 0) & (candidate < TILE_COUNT)
    random_part = jax.random.randint(stream, (TILE_COUNT, span_tiles), 0, 1 << 20)
    own_tile = candidate == jnp.arange(TILE_COUNT, dtype=jnp.int32)[:, None]
    ranking = jnp.where(own_tile, (1 << 20) * span_tiles + position[None, :], random_part * span_tiles + position[None, :])
    ranking = jnp.where(inside, ranking, -1 - position[None, :])
    picked_vals, picked = lax.top_k(ranking, MAXB)
    return jnp.take_along_axis(candidate, picked, axis=1).astype(jnp.int32)


def draw_block_count(key, part):
    stream = jax.random.fold_in(key, 53)
    keys = jax.random.split(stream, 3)
    devices = TILE_COUNT // TILES_DEV
    lowest = jax.random.randint(keys[0], (devices,), 1, MAXB + 1)
    lowest_rows = jnp.repeat(lowest, TILES_DEV)
    spread = jax.random.randint(keys[1], (TILE_COUNT,), 0, 1 << 20)
    counted = lowest_rows + spread % (MAXB + 1 - lowest_rows)
    full_tile = jax.random.randint(keys[2], (), 0, TILE_COUNT)
    counted = jnp.where(jnp.arange(TILE_COUNT, dtype=jnp.int32) == full_tile, MAXB, counted)
    return counted.astype(jnp.int32)


def length_profile(amount, total, most, slope):
    portions = [(1 << 20) // math.isqrt(standing ** slope) + 1 for standing in range(2, amount + 1)]
    spare, given = total - most - (amount - 1), [1] * (amount - 1)
    while spare > 0:
        candidates = [i for i in range(amount - 1) if given[i] < most]
        pool, left = sum([portions[i] for i in candidates]), spare
        for i in candidates:
            addition = min(most - given[i], max(1, left * portions[i] // pool), spare)
            given[i] = given[i] + addition
            spare = spare - addition
    return np.array([most] + given)


def uneven(rng, count, total, reach, skew):
    if count == 2:
        one = jax.random.randint(rng, (), max(1, total - reach), min(reach, total - 1) + 1)
        return jnp.stack([one, total - one])
    tallies = jnp.asarray(length_profile(count, total, reach, skew), jnp.int32)
    couples = (count - 1) // 2
    donor, taker = tallies[1:1 + 2 * couples:2], tallies[2:2 + 2 * couples:2]
    margin = jnp.minimum(donor - 1, reach - taker)
    passed = jax.random.randint(jax.random.fold_in(rng, 1), (couples,), 0, 1 << 20) % (margin + 1)
    tallies = tallies.at[1:1 + 2 * couples:2].set(donor - passed).at[2:2 + 2 * couples:2].set(taker + passed)
    return tallies[jax.random.permutation(jax.random.fold_in(rng, 2), count)]


def gaussian(own_key, dims, deviation, reach, kind=jnp.bfloat16):
    return jnp.clip(deviation * jax.random.normal(own_key, dims, jnp.float32), -reach, reach).astype(kind)


def setup_inputs(seed: int = 0, part: int = 0) -> dict:
    arg_keys = jax.random.split(jax.random.key(seed), 9)
    part_keys = jax.random.split(jax.random.fold_in(arg_keys[8], part), 9)
    return {
        "source_emb": draw_source_emb(jax.random.fold_in(jax.random.fold_in(arg_keys[8], part), 71), part),
        "target_emb": draw_target_emb(jax.random.fold_in(jax.random.fold_in(arg_keys[8], part), 71), part),
        "source_cluster": jnp.searchsorted(jnp.cumsum(uneven(part_keys[2], CLUSTERS, SOURCES, 2 * SOURCES // CLUSTERS, 1)), jnp.arange(SOURCES), side="right").astype(jnp.int32),
        "target_cluster": jnp.searchsorted(jnp.cumsum(uneven(part_keys[3], CLUSTERS, TARGETS, 2 * TARGETS // CLUSTERS, 1)), jnp.arange(TARGETS), side="right").astype(jnp.int32),
        "coarse_source": gaussian(part_keys[4], (CLUSTERS,), 0.5, 3.0, jnp.float32),
        "coarse_target": gaussian(part_keys[5], (CLUSTERS,), 0.5, 3.0, jnp.float32),
        "block_list": draw_block_list(jax.random.fold_in(jax.random.fold_in(arg_keys[8], part), 71), part),
        "block_count": draw_block_count(jax.random.fold_in(jax.random.fold_in(arg_keys[8], part), 71), part),
    }


EPSILON = 0.5
NEGATIVE = -1e30


def stable_lse(values, reduce_dim):
    highest = jnp.max(values, axis=reduce_dim, keepdims=True)
    return jnp.squeeze(highest, reduce_dim) + jnp.log(jnp.sum(jnp.exp(values - highest), axis=reduce_dim))


def reference(source_emb, target_emb, source_cluster, target_cluster, coarse_source, coarse_target, block_list, block_count):
    source_pot = jnp.take(coarse_source, source_cluster).astype(jnp.float32)
    target_pot = jnp.take(coarse_target, target_cluster).astype(jnp.float32)
    source_tiles = source_emb.reshape(TILE_COUNT, TILE, EMBED)
    target_tiles = target_emb.reshape(TILE_COUNT, TILE, EMBED)
    live = jnp.arange(MAXB, dtype=jnp.int32)[None, :] < block_count[:, None]
    for iteration in range(ITERS):
        target_grid = target_pot.reshape(TILE_COUNT, TILE)
        source_grid = source_pot.reshape(TILE_COUNT, TILE)

        def one_tile(inputs):
            source_block, source_row_pot, listed, active = inputs
            chosen = jnp.take(target_tiles, listed, axis=0).astype(jnp.float32)
            scores = jnp.einsum("re,bce->brc", source_block.astype(jnp.float32), chosen, precision=lax.Precision.HIGHEST)
            row_terms = (jnp.take(target_grid, listed, axis=0)[:, None, :] + scores) / EPSILON
            row_terms = jnp.where(active[:, None, None], row_terms, NEGATIVE)
            row_lse = stable_lse(jnp.transpose(row_terms, (1, 0, 2)).reshape(TILE, MAXB * TILE), 1)
            col_terms = (source_row_pot[None, :, None] + scores) / EPSILON
            col_part = jnp.where(active[:, None], stable_lse(col_terms, 1), NEGATIVE)
            return row_lse, col_part

        row_lse, col_part = lax.map(one_tile, (source_tiles, source_grid, block_list, live))
        col_top = jnp.full((TILE_COUNT, TILE), NEGATIVE, jnp.float32).at[block_list].max(col_part)
        col_total = jnp.zeros((TILE_COUNT, TILE), jnp.float32).at[block_list].add(jnp.exp(col_part - col_top[block_list]))
        col_lse = col_top + jnp.log(col_total)
        source_next = 0.5 * (source_pot + EPSILON * jnp.log(jnp.float32(TARGETS)) - EPSILON * row_lse.reshape(SOURCES))
        target_next = 0.5 * (target_pot + EPSILON * jnp.log(jnp.float32(SOURCES)) - EPSILON * col_lse.reshape(TARGETS))
        source_pot, target_pot = source_next, target_next
    return source_pot, target_pot
```

```python
import functools
import math

import jax
import jax.numpy as jnp
from jax import lax
from jax.experimental import pallas as pl
from jax.experimental.pallas import tpu as pltpu
from jax.sharding import PartitionSpec as P

TILE = 128
ITERS = 2
EPSILON = 0.5
NEGATIVE = -1e30
SCALE = 1.0 / (EPSILON * math.log(2.0))
LAST = 12
MESH = pl.DeviceIdType.MESH
VM = pltpu.VMEM
F32 = jnp.float32
SPEC = pl.BlockSpec(memory_space=pltpu.VMEM)
SMEM = pl.BlockSpec(memory_space=pltpu.SMEM)
ANY = pl.BlockSpec(memory_space=pl.ANY)
NT = (((1,), (1,)), ((), ()))
LO, HI = 1e-8, 1e20
FAR = 15.0


def partners(n):
    me = lax.axis_index("row")
    odd = lax.rem(me, 2)
    fast = me + 1 - 2 * odd
    slow = lax.rem(me - 1 + 2 * odd + n, n)
    return me, odd, fast, slow


def place(listed, me, odd, tiles):
    w = listed - (me - 1) * tiles
    turned = jnp.where(w >= 2 * tiles, w - 2 * tiles, jnp.where(w < tiles, w + 2 * tiles, w))
    return jnp.where(odd == 1, w, turned)


def greet(devices):
    barrier = pltpu.get_barrier_semaphore()
    for d in devices:
        pl.semaphore_signal(barrier, inc=1, device_id={"row": d}, device_id_type=MESH)
    pl.semaphore_wait(barrier, len(devices))


def remote(src, dst, sems, i, device):
    send, recv = sems
    return pltpu.make_async_remote_copy(
        src_ref=src,
        dst_ref=dst,
        send_sem=send.at[i],
        recv_sem=recv.at[i],
        device_id={"row": device},
        device_id_type=MESH,
    )


def three(x):
    a = x.astype(jnp.bfloat16)
    rest = x - a.astype(F32)
    b = rest.astype(jnp.bfloat16)
    c = (rest - b.astype(F32)).astype(jnp.bfloat16)
    return a, b, c


def add_up(onehot, parts):
    a, b, c = three(parts)
    dot = lambda y: jnp.dot(onehot, y, preferred_element_type=F32)
    return dot(a) + (dot(b) + dot(c))


def kernel_a(
    n, tiles, maxb,
    bl, bc, src, tgt, scl, tcl, ctab_s, ctab_t,
    k_ref, ra_ref, p1_ref, f0b_ref, g0_ref, x_ref, of_ref, es1_ref, es2_ref, oh_ref, lst_ref,
    ids_ref, tab_ref, f0_ref, oht_ref, ft_ref, send, recv, local,
):
    me, odd, fast, slow = partners(n)
    sems = (send, recv)
    first = tiles - LAST
    greet((fast, slow))
    copies = [
        remote(tcl, ids_ref.at[pl.ds(2 * tiles, tiles)], sems, 0, slow),
        remote(tcl, ids_ref.at[pl.ds(0, tiles)], sems, 1, fast),
        remote(tgt.at[pl.ds(0, first)], es1_ref, sems, 2, slow),
        remote(tgt.at[pl.ds(first, LAST)], es2_ref, sems, 3, slow),
        remote(tgt, of_ref.at[pl.ds(0, tiles)], sems, 4, fast),
    ]
    for c in copies:
        c.start()
    mine = [
        pltpu.make_async_copy(tcl, ids_ref.at[pl.ds(tiles, tiles)], local.at[0]),
        pltpu.make_async_copy(scl, ids_ref.at[pl.ds(3 * tiles, tiles)], local.at[1]),
        pltpu.make_async_copy(src, x_ref, local.at[2]),
        pltpu.make_async_copy(tgt, of_ref.at[pl.ds(tiles, tiles)], local.at[3]),
    ]
    for c in mine:
        c.start()

    for q, tab in enumerate((ctab_s, ctab_t)):
        wide = jnp.concatenate([tab[...], jnp.zeros((TILE - tab.shape[0], TILE), F32)], axis=0)
        turned = jnp.transpose(wide)[:, : tab.shape[0]]
        tab_ref[q] = jnp.concatenate(three(turned), axis=1)

    flat = lax.broadcasted_iota(jnp.int32, (8, TILE), 0) * TILE + lax.broadcasted_iota(
        jnp.int32, (8, TILE), 1
    )
    lane = lax.broadcasted_iota(jnp.int32, (maxb, TILE), 1)
    sub = lax.broadcasted_iota(jnp.int32, (maxb, TILE), 0)

    def order(t, carry):
        lst, count = carry
        active = bc[t]
        where_to = jnp.full((maxb, TILE), -1, jnp.int32)
        for k in range(maxb):
            r = place(bl[t, k], me, odd, tiles)
            on = jnp.where(k < active, 1, 0)
            late = on * jnp.where(r >= 2 * tiles + first, 1, 0)
            lst = lst + jnp.where(flat == count, (t * maxb + k) * late, 0)
            count = count + late
            where_to = jnp.where(sub == k, r * on - (1 - on), where_to)
        oht_ref[pl.ds(pl.multiple_of(t * maxb, maxb), maxb), :] = jnp.where(
            lane == where_to, 1.0, 0.0
        )
        return lst, count

    lst, count = lax.fori_loop(0, tiles, order, (jnp.zeros((8, TILE), jnp.int32), 0))
    lst_ref[...] = jnp.where(flat == 8 * TILE - 1, count, lst)
    oh_ref[...] = jnp.transpose(oht_ref[...]).astype(jnp.bfloat16)

    low = lax.broadcasted_iota(jnp.int32, (TILE, TILE), 0)
    high = lax.broadcasted_iota(jnp.int32, (tiles, TILE), 0)

    def look_up(row, q):
        ids = ids_ref[pl.ds(row, 1), :]
        hit = jnp.where(high == lax.shift_right_logical(ids, 7), 1.0, 0.0).astype(jnp.bfloat16)
        got = jnp.dot(
            tab_ref[q], jnp.concatenate([hit, hit, hit], axis=0), preferred_element_type=F32
        )
        return jnp.sum(jnp.where(low == (ids & 127), got, 0.0), axis=0, keepdims=True)

    mine[0].wait()
    mine[1].wait()

    def own_rows(i, _):
        for u in range(4):
            t = i * 4 + u
            f0_ref[pl.ds(t, 1), :] = look_up(3 * tiles + t, 0)
            g0_ref[pl.ds(tiles + t, 1), :] = look_up(tiles + t, 1)
        return 0

    lax.fori_loop(0, tiles // 4, own_rows, 0)
    ft_ref[...] = jnp.transpose(
        jnp.concatenate([f0_ref[...], jnp.zeros((TILE - tiles, TILE), F32)], axis=0)
    )
    lanes = lax.broadcasted_iota(jnp.int32, (TILE, TILE), 1)

    def spread(i, _):
        for u in range(2):
            t = i * 2 + u
            col = jnp.sum(jnp.where(lanes == t, ft_ref[...], 0.0), axis=1, keepdims=True)
            f0b_ref[t] = jnp.broadcast_to(col, (TILE, TILE))
        return 0

    lax.fori_loop(0, tiles // 2, spread, 0)
    copies[0].wait_recv()
    copies[1].wait_recv()

    def other_rows(i, _):
        for u in range(4):
            t = i * 4 + u
            g0_ref[pl.ds(t, 1), :] = look_up(t, 1)
            g0_ref[pl.ds(2 * tiles + t, 1), :] = look_up(2 * tiles + t, 1)
        return 0

    lax.fori_loop(0, tiles // 4, other_rows, 0)
    mine[2].wait()
    mine[3].wait()
    copies[4].wait_recv()

    def near(t, _):
        x = x_ref[t]
        active = bc[t]
        for k in range(0, maxb, 2):
            ys, bias = [], []
            for u in range(2):
                r = place(bl[t, k + u], me, odd, tiles)
                ys.append(of_ref[jnp.clip(r, 0, 2 * tiles - 1)])
                on = jnp.where(k + u < active, 1, 0) * jnp.where(r < 2 * tiles, 1, 0)
                bias.append(jnp.where(on == 1, 0.0, NEGATIVE).astype(F32))
            s = lax.dot_general(x, jnp.concatenate(ys, axis=0), NT, preferred_element_type=F32)
            for u in range(2):
                part = s[:, u * TILE : (u + 1) * TILE]
                k_ref[t * maxb + k + u] = jnp.exp2(part * SCALE + bias[u])
        return 0

    lax.fori_loop(0, tiles, near, 0)
    copies[2].wait_recv()

    def middle(t, _):
        x = x_ref[t]
        active = bc[t]
        b0 = jnp.exp2(f0b_ref[t] * SCALE)
        rows = jnp.zeros((TILE, TILE), F32)
        cols = []
        for k in range(0, maxb, 2):
            ys, bias, at = [], [], []
            for u in range(2):
                r = place(bl[t, k + u], me, odd, tiles)
                at.append(jnp.clip(r, 0, 3 * tiles - 1))
                inner = r - 2 * tiles
                ys.append(es1_ref[jnp.clip(inner, 0, first - 1)])
                on = (
                    jnp.where(k + u < active, 1, 0)
                    * jnp.where(inner >= 0, 1, 0)
                    * jnp.where(inner < first, 1, 0)
                )
                bias.append(jnp.where(on == 1, 0.0, NEGATIVE).astype(F32))
            s = lax.dot_general(x, jnp.concatenate(ys, axis=0), NT, preferred_element_type=F32)
            for u in range(2):
                part = s[:, u * TILE : (u + 1) * TILE]
                p = t * maxb + k + u
                kv = k_ref[p] + jnp.exp2(part * SCALE + bias[u])
                k_ref[p] = kv
                rows = rows + kv * jnp.exp2(g0_ref[pl.ds(at[u], 1), :] * SCALE)
                cols.append(jnp.sum(kv * b0, axis=0, keepdims=True))
        ra_ref[t] = rows
        p1_ref[pl.ds(pl.multiple_of(t * maxb, maxb), maxb), :] = jnp.concatenate(cols, axis=0)
        return 0

    lax.fori_loop(0, tiles, middle, 0)
    copies[3].wait_recv()
    for c in copies:
        c.wait_send()


def fetch(r, ybuf, of_ref, es1_ref, es2_ref, tiles):
    first = tiles - LAST

    @pl.when(r < 2 * tiles)
    def _():
        ybuf[...] = of_ref[jnp.minimum(r, 2 * tiles - 1)]

    @pl.when((r >= 2 * tiles) & (r < 2 * tiles + first))
    def _():
        ybuf[...] = es1_ref[jnp.clip(r - 2 * tiles, 0, first - 1)]

    @pl.when(r >= 2 * tiles + first)
    def _():
        ybuf[...] = es2_ref[jnp.clip(r - 2 * tiles - first, 0, LAST - 1)]


def kernel_b(
    n, tiles, maxb, log_size,
    bl, bc, lst, k_in, ra_in, p1_in, f0b_ref, g0_ref, x_ref, of_ref, es1_ref, es2_ref, oh_ref,
    k_ref, ra_ref, p1_ref, f1b_ref, c1_ref, c2_ref, bad_ref,
    ybuf, cols,
):
    me, odd, fast, slow = partners(n)
    first = tiles - LAST
    pairs = tiles * maxb
    count = lst[7, TILE - 1]
    wide = 4

    def late(i, _):
        for u in range(wide):
            at = i * wide + u
            ok = at < count
            p = lst[lax.shift_right_logical(at, 7), at & 127]
            t = lax.div(p, maxb)
            r = place(bl[t, lax.rem(p, maxb)], me, odd, tiles)
            r = jnp.clip(r, 0, 3 * tiles - 1)
            y = es2_ref[jnp.clip(r - 2 * tiles - first, 0, LAST - 1)]
            s = lax.dot_general(x_ref[t], y, NT, preferred_element_type=F32)
            kv = jnp.exp2(s * SCALE + jnp.where(ok, 0.0, NEGATIVE).astype(F32))
            b0 = jnp.exp2(f0b_ref[t] * SCALE)
            a0 = jnp.exp2(g0_ref[pl.ds(r, 1), :] * SCALE)
            ra_ref[t] = ra_ref[t] + kv * a0
            p1_ref[pl.ds(p, 1), :] = p1_ref[pl.ds(p, 1), :] + jnp.sum(
                kv * b0, axis=0, keepdims=True
            )
            k_ref[p] = k_ref[p] + kv
        return 0

    lax.fori_loop(0, lax.div(count + wide - 1, wide), late, 0)

    def finish(i, worst):
        for u in range(4):
            t = i * 4 + u
            total = jnp.sum(ra_ref[t], axis=1, keepdims=True)
            worst = jnp.maximum(worst, jnp.where((total >= LO) & (total <= HI), 0.0, 1.0))
            lse = jnp.broadcast_to(jnp.log(total), (TILE, TILE))
            f1b_ref[t] = 0.5 * (f0b_ref[t] + log_size - EPSILON * lse)
        return worst

    worst = lax.fori_loop(0, tiles // 4, finish, jnp.zeros((TILE, 1), F32))
    onehot = oh_ref[...]
    here = jnp.sum(onehot.astype(F32), axis=1, keepdims=True) > 0.5
    total = add_up(onehot, p1_ref[...])
    fits = (total >= LO) & (total <= HI)
    c1_ref[...] = jnp.where(here, jnp.log(total), NEGATIVE)[: 3 * tiles]
    wrong = jnp.where(here & jnp.logical_not(fits), 1.0, 0.0)
    bad = jnp.maximum(jnp.max(worst), jnp.max(wrong))
    bad_ref[...] = jnp.full((8, TILE), bad)
    c2_ref[...] = jnp.full((3 * tiles, TILE), NEGATIVE, F32)

    @pl.when(bad > 0.5)
    def _():
        for c in range(4):
            cols[c] = jnp.full((3 * tiles, TILE), NEGATIVE if c % 2 == 0 else 0.0, F32)

        def column(c, r, terms):
            top = cols[c, pl.ds(r, 1), :]
            now = jnp.maximum(top, jnp.max(terms, axis=0, keepdims=True))
            cols[c + 1, pl.ds(r, 1), :] = cols[c + 1, pl.ds(r, 1), :] * jnp.exp(top - now) + jnp.sum(
                jnp.exp(terms - now), axis=0, keepdims=True
            )
            cols[c, pl.ds(r, 1), :] = now

        def one(t, _):
            x = x_ref[t]
            f0 = f0b_ref[t]

            def slot(k, carry):
                top, total = carry
                r = place(bl[t, k], me, odd, tiles)
                fetch(r, ybuf, of_ref, es1_ref, es2_ref, tiles)
                s = lax.dot_general(x, ybuf[...], NT, preferred_element_type=F32)
                terms = (g0_ref[pl.ds(r, 1), :] + s) / EPSILON
                now = jnp.maximum(top, jnp.max(terms, axis=1, keepdims=True))
                total = total * jnp.exp(top - now) + jnp.sum(
                    jnp.exp(terms - now), axis=1, keepdims=True
                )
                column(0, r, (f0 + s) / EPSILON)
                return now, total

            top, total = lax.fori_loop(
                0, bc[t], slot, (jnp.full((TILE, 1), NEGATIVE, F32), jnp.zeros((TILE, 1), F32))
            )
            lse = jnp.broadcast_to(top + jnp.log(total), (TILE, TILE))
            f1 = 0.5 * (f0 + log_size - EPSILON * lse)
            f1b_ref[t] = f1

            def again(k, _):
                r = place(bl[t, k], me, odd, tiles)
                fetch(r, ybuf, of_ref, es1_ref, es2_ref, tiles)
                s = lax.dot_general(x, ybuf[...], NT, preferred_element_type=F32)
                column(2, r, (f1b_ref[t] + s) / EPSILON)
                return 0

            lax.fori_loop(0, bc[t], again, 0)
            return 0

        lax.fori_loop(0, tiles, one, 0)
        c1_ref[...] = jnp.where(cols[1] > 0, cols[0] + jnp.log(cols[1]), NEGATIVE)
        c2_ref[...] = jnp.where(cols[3] > 0, cols[2] + jnp.log(cols[3]), NEGATIVE)


def merge(*parts):
    top = functools.reduce(jnp.maximum, parts)
    return top + jnp.log(functools.reduce(jnp.add, [jnp.exp(p - top) for p in parts]))


def kernel_f(
    n, tiles, maxb, log_size,
    bl, k_ref, f1b_ref, g0_ref, oh_ref, c1_ref, c2s_ref, bad_ref,
    f2_ref, g2_ref, g1_ref,
    p2_ref, c2_ref, a1_ref, ft_ref, got_f, got_s, got_fs, got_sf, got2_f, got2_s, send, recv,
):
    me, odd, fast, slow = partners(n)
    beyond_fast = lax.rem(fast - 1 + 2 * (1 - odd) + n, n)
    beyond_slow = slow - 1 + 2 * odd
    sems = (send, recv)
    greet((fast, slow, beyond_fast, beyond_slow))
    copies = [
        remote(c1_ref.at[pl.ds(tiles, 2 * tiles)], got_s, sems, 0, slow),
        remote(c1_ref.at[pl.ds(0, tiles)], got_sf, sems, 1, beyond_fast),
        remote(c1_ref.at[pl.ds(2 * tiles, tiles)], got_fs, sems, 2, beyond_slow),
        remote(c1_ref.at[pl.ds(0, 2 * tiles)], got_f, sems, 3, fast),
    ]
    for c in copies:
        c.start()

    def columns(t, _):
        b1 = jnp.exp2(f1b_ref[t] * SCALE)
        p2_ref[pl.ds(pl.multiple_of(t * maxb, maxb), maxb), :] = jnp.concatenate(
            [jnp.sum(k_ref[t * maxb + k] * b1, axis=0, keepdims=True) for k in range(maxb)], axis=0
        )
        return 0

    lax.fori_loop(0, tiles, columns, 0)
    total = add_up(oh_ref[...], p2_ref[...])[: 3 * tiles]
    quick = jnp.where(total > 0, jnp.log(total), NEGATIVE)
    c2_ref[...] = jnp.where(bad_ref[0:1, :] > 0.5, c2s_ref[...], quick)

    for c in copies:
        c.wait_recv()
    own = pl.ds(tiles, tiles)
    front, back = pl.ds(0, tiles), pl.ds(2 * tiles, tiles)
    second = pl.ds(tiles, tiles)
    for part, lse in (
        (front, merge(c1_ref[front, :], got_f[second, :], got_fs[...])),
        (own, merge(c1_ref[own, :], got_f[front, :], got_s[second, :])),
        (back, merge(c1_ref[back, :], got_s[front, :], got_sf[...])),
    ):
        g1 = 0.5 * (g0_ref[part, :] + log_size - EPSILON * lse)
        g1_ref[part, :] = g1
        a1_ref[part, :] = jnp.exp2(g1 * SCALE)
    final = [
        remote(c2_ref.at[back], got2_s, sems, 4, slow),
        remote(c2_ref.at[front], got2_f, sems, 5, fast),
    ]
    for c in final:
        c.start()

    lanes = lax.broadcasted_iota(jnp.int32, (TILE, TILE), 1)
    ft_ref[...] = jnp.zeros((TILE, TILE), F32)

    def rows(t, _):
        total = jnp.zeros((TILE, TILE), F32)
        for k in range(maxb):
            r = jnp.clip(place(bl[t, k], me, odd, tiles), 0, 3 * tiles - 1)
            total = total + k_ref[t * maxb + k] * a1_ref[pl.ds(r, 1), :]
        total = jnp.sum(total, axis=1, keepdims=True)
        fits = (total >= LO) & (total <= HI)
        lse = jnp.broadcast_to(jnp.log(jnp.where(fits, total, jnp.nan)), (TILE, TILE))
        f2 = 0.5 * (f1b_ref[t] + log_size - EPSILON * lse)
        ft_ref[...] = jnp.where(lanes == t, f2, ft_ref[...])
        return 0

    lax.fori_loop(0, tiles, rows, 0)
    f2_ref[...] = jnp.transpose(ft_ref[...])[:tiles]
    for c in final:
        c.wait_recv()
    lse = merge(c2_ref[own, :], got2_f[...], got2_s[...])
    g2_ref[...] = 0.5 * (g1_ref[own, :] + log_size - EPSILON * lse)
    for c in copies + final:
        c.wait_send()


def kernel_g(
    n, tiles, maxb, log_size,
    bl, bc, f2_in, g2_in, g1_ref, bad_ref, f1b_ref, x_ref, of_ref, es1_ref, es2_ref,
    f2_ref, g2_ref, ft_ref, ybuf,
):
    me, odd, fast, slow = partners(n)
    f2 = f2_in[...]
    f2_ref[...] = f2
    g2_ref[...] = g2_in[...]
    odd_one = jnp.where(f2 == f2, 0.0, 1.0)
    bad = jnp.maximum(
        jnp.maximum(jnp.max(odd_one), jnp.max(bad_ref[...])),
        jnp.max(jnp.where(jnp.abs(g1_ref[...]) <= FAR, 0.0, 1.0)),
    )

    @pl.when(bad > 0.5)
    def _():
        lanes = lax.broadcasted_iota(jnp.int32, (TILE, TILE), 1)
        ft_ref[...] = jnp.zeros((TILE, TILE), F32)

        def one(t, _):
            x = x_ref[t]

            def slot(k, carry):
                top, total = carry
                r = place(bl[t, k], me, odd, tiles)
                fetch(r, ybuf, of_ref, es1_ref, es2_ref, tiles)
                s = lax.dot_general(x, ybuf[...], NT, preferred_element_type=F32)
                terms = (g1_ref[pl.ds(r, 1), :] + s) / EPSILON
                now = jnp.maximum(top, jnp.max(terms, axis=1, keepdims=True))
                total = total * jnp.exp(top - now) + jnp.sum(
                    jnp.exp(terms - now), axis=1, keepdims=True
                )
                return now, total

            top, total = lax.fori_loop(
                0, bc[t], slot, (jnp.full((TILE, 1), NEGATIVE, F32), jnp.zeros((TILE, 1), F32))
            )
            lse = jnp.broadcast_to(top + jnp.log(total), (TILE, TILE))
            f2 = 0.5 * (f1b_ref[t] + log_size - EPSILON * lse)
            ft_ref[...] = jnp.where(lanes == t, f2, ft_ref[...])
            return 0

        lax.fori_loop(0, tiles, one, 0)
        f2_ref[...] = jnp.transpose(ft_ref[...])[:tiles]


def shards(n, src, tgt, scl, tcl, cs, ct, bl, bc):
    rows, width = src.shape
    tiles = rows // TILE
    maxb = bl.shape[1]
    first = tiles - LAST
    log_size = EPSILON * math.log(rows * n)
    bf = jnp.bfloat16
    cost = lambda flops: pl.CostEstimate(flops=flops, bytes_accessed=1 << 23, transcendentals=0)
    flops = 2 * tiles * maxb * TILE * TILE * width
    by_tile = lambda a: a.reshape(tiles, TILE, width)
    rows_of = lambda a: a.reshape(tiles, TILE)
    table = lambda a: a.reshape(a.shape[0] // TILE, TILE)
    hold = VM if KEEP else jax.ShapeDtypeStruct
    k, ra, p1, f0b, g0, x, of, es1, es2, oh, lst = pl.pallas_call(
        functools.partial(kernel_a, n, tiles, maxb),
        out_shape=(
            hold((tiles * maxb, TILE, TILE), F32),
            hold((tiles, TILE, TILE), F32),
            hold((tiles * maxb, TILE), F32),
            hold((tiles, TILE, TILE), F32),
            hold((3 * tiles, TILE), F32),
            hold((tiles, TILE, width), bf),
            hold((2 * tiles, TILE, width), bf),
            hold((first, TILE, width), bf),
            hold((LAST, TILE, width), bf),
            hold((TILE, tiles * maxb), bf),
            jax.ShapeDtypeStruct((8, TILE), jnp.int32),
        ),
        in_specs=[SMEM, SMEM, ANY, ANY, ANY, ANY, SPEC, SPEC],
        out_specs=(SPEC,) * 11,
        scratch_shapes=[
            VM((4 * tiles, TILE), jnp.int32),
            VM((2, TILE, 3 * tiles), bf),
            VM((tiles, TILE), F32),
            VM((tiles * maxb, TILE), F32),
            VM((TILE, TILE), F32),
            pltpu.SemaphoreType.DMA((5,)),
            pltpu.SemaphoreType.DMA((5,)),
            pltpu.SemaphoreType.DMA((4,)),
        ],
        compiler_params=pltpu.CompilerParams(
            collective_id=0, has_side_effects=True, vmem_limit_bytes=LIMIT
        ),
        cost_estimate=cost(2 * flops),
        name="exchange",
    )(bl, bc, by_tile(src), by_tile(tgt), rows_of(scl), rows_of(tcl), table(cs), table(ct))

    k, ra, p1, f1b, c1, c2s, bad = pl.pallas_call(
        functools.partial(kernel_b, n, tiles, maxb, log_size),
        out_shape=(
            hold((tiles * maxb, TILE, TILE), F32),
            hold((tiles, TILE, TILE), F32),
            hold((tiles * maxb, TILE), F32),
            hold((tiles, TILE, TILE), F32),
            hold((3 * tiles, TILE), F32),
            hold((3 * tiles, TILE), F32),
            hold((8, TILE), F32),
        ),
        in_specs=[SMEM, SMEM, SMEM] + [SPEC] * 10,
        out_specs=(SPEC,) * 7,
        scratch_shapes=[
            VM((TILE, width), bf),
            VM((4, 3 * tiles, TILE), F32),
        ],
        input_output_aliases={3: 0, 4: 1, 5: 2},
        compiler_params=pltpu.CompilerParams(vmem_limit_bytes=LIMIT),
        cost_estimate=cost(flops),
        name="last_pairs",
    )(bl, bc, lst, k, ra, p1, f0b, g0, x, of, es1, es2, oh)

    f2, g2, g1 = pl.pallas_call(
        functools.partial(kernel_f, n, tiles, maxb, log_size),
        out_shape=(
            hold((tiles, TILE), F32),
            hold((tiles, TILE), F32),
            hold((3 * tiles, TILE), F32),
        ),
        in_specs=[SMEM] + [SPEC] * 7,
        out_specs=(SPEC,) * 3,
        scratch_shapes=[
            VM((tiles * maxb, TILE), F32),
            VM((3 * tiles, TILE), F32),
            VM((3 * tiles, TILE), F32),
            VM((TILE, TILE), F32),
            VM((2 * tiles, TILE), F32),
            VM((2 * tiles, TILE), F32),
            VM((tiles, TILE), F32),
            VM((tiles, TILE), F32),
            VM((tiles, TILE), F32),
            VM((tiles, TILE), F32),
            pltpu.SemaphoreType.DMA((6,)),
            pltpu.SemaphoreType.DMA((6,)),
        ],
        compiler_params=pltpu.CompilerParams(
            collective_id=1, has_side_effects=True, vmem_limit_bytes=LIMIT
        ),
        cost_estimate=cost(flops),
        name="potentials",
    )(bl, k, f1b, g0, oh, c1, c2s, bad)

    f2, g2 = pl.pallas_call(
        functools.partial(kernel_g, n, tiles, maxb, log_size),
        out_shape=(jax.ShapeDtypeStruct((tiles, TILE), F32),) * 2,
        in_specs=[SMEM, SMEM] + [SPEC] * 9,
        out_specs=(SPEC,) * 2,
        scratch_shapes=[VM((TILE, TILE), F32), VM((TILE, width), bf)],
        compiler_params=pltpu.CompilerParams(vmem_limit_bytes=LIMIT),
        cost_estimate=cost(flops),
        name="guard",
    )(bl, bc, f2, g2, g1, bad, f1b, x, of, es1, es2)
    return f2.reshape(rows), g2.reshape(rows)


KEEP = True
LIMIT = 14 << 20


def solution(mesh):
    both = P(("grp", "row"))
    wide = P(("grp", "row"), None)
    return jax.shard_map(
        functools.partial(shards, mesh.shape["row"]),
        mesh=mesh,
        in_specs=(wide, wide, both, both, P("grp"), P("grp"), wide, both),
        out_specs=(both, both),
        check_vma=False,
    )
```

```python
import functools
import math

import jax
import jax.numpy as jnp
from jax import lax
from jax.experimental import pallas as pl
from jax.experimental.pallas import tpu as pltpu
from jax.sharding import PartitionSpec as P

TILE = 128
ITERS = 2
EPSILON = 0.5
NEGATIVE = -1e30
SCALE = 1.0 / (EPSILON * math.log(2.0))
WIDE = 8
MESH = pl.DeviceIdType.MESH
VM = pltpu.VMEM
F32 = jnp.float32
SPEC = pl.BlockSpec(memory_space=pltpu.VMEM)
SMEM = pl.BlockSpec(memory_space=pltpu.SMEM)
ANY = pl.BlockSpec(memory_space=pl.ANY)
FAR_MEM = pl.BlockSpec(memory_space=pltpu.HBM)
NT = (((1,), (1,)), ((), ()))
LO, HI = 1e-8, 1e20
FAR = 15.0


def partners(n):
    me = lax.axis_index("row")
    odd = lax.rem(me, 2)
    slow = me - 1 + 2 * odd
    return me, odd, me + 1 - 2 * odd, slow, (slow >= 0) & (slow < n)


def place(listed, me, odd, tiles):
    w = listed - (me - 1) * tiles
    turned = jnp.where(w >= 2 * tiles, w - 2 * tiles, jnp.where(w < tiles, w + 2 * tiles, w))
    return jnp.where(odd == 1, w, turned)


def greet(device):
    pl.semaphore_signal(
        pltpu.get_barrier_semaphore(), inc=1, device_id={"row": device}, device_id_type=MESH
    )


def remote(src, dst, sems, i, device):
    send, recv = sems
    return pltpu.make_async_remote_copy(
        src_ref=src,
        dst_ref=dst,
        send_sem=send.at[i],
        recv_sem=recv.at[i],
        device_id={"row": device},
        device_id_type=MESH,
    )


def three(x):
    a = x.astype(jnp.bfloat16)
    rest = x - a.astype(F32)
    b = rest.astype(jnp.bfloat16)
    c = (rest - b.astype(F32)).astype(jnp.bfloat16)
    return a, b, c


def add_up(onehot, parts):
    a, b, c = three(parts)
    dot = lambda y: jnp.dot(onehot, y, preferred_element_type=F32)
    return dot(a) + (dot(b) + dot(c))


def kernel_a(
    n, tiles, maxb,
    bl_hbm, bc_hbm, src, tgt, scl, tcl, cs_hbm, ct_hbm,
    ft_ref, g0_ref, a0_ref, x_ref, of_ref, oh_ref, lst_ref,
    bl, bc, ids_ref, ctab_ref, tab_ref, f0_ref, oht_ref, send, recv, local,
):
    me, odd, fast, slow, has_slow = partners(n)
    sems = (send, recv)
    here = [
        pltpu.make_async_copy(bl_hbm, bl, local.at[0]),
        pltpu.make_async_copy(bc_hbm, bc, local.at[1]),
        pltpu.make_async_copy(cs_hbm, ctab_ref.at[0], local.at[2]),
        pltpu.make_async_copy(ct_hbm, ctab_ref.at[1], local.at[3]),
        pltpu.make_async_copy(tcl, ids_ref.at[pl.ds(tiles, tiles)], local.at[4]),
        pltpu.make_async_copy(scl, ids_ref.at[pl.ds(3 * tiles, tiles)], local.at[5]),
        pltpu.make_async_copy(tgt, of_ref.at[pl.ds(tiles, tiles)], local.at[6]),
        pltpu.make_async_copy(src, x_ref, local.at[7]),
    ]
    past_fast, past_slow = fast + 1 - 2 * odd, slow - 1 + 2 * odd
    has_past = (past_fast >= 0) & (past_fast < n)
    greet(fast)

    @pl.when(has_past)
    def _():
        greet(past_fast)

    @pl.when(has_slow)
    def _():
        greet(past_slow)

    for c in here:
        c.start()
    pl.semaphore_wait(
        pltpu.get_barrier_semaphore(), 1 + jnp.where(has_slow, 1, 0) + jnp.where(has_past, 1, 0)
    )
    near = [
        remote(tcl, ids_ref.at[pl.ds(0, tiles)], sems, 0, fast),
        remote(tgt, of_ref.at[pl.ds(0, tiles)], sems, 1, fast),
    ]
    onward = remote(
        ids_ref.at[pl.ds(0, tiles)], ids_ref.at[pl.ds(2 * tiles, tiles)], sems, 2, past_fast
    )
    for c in near:
        c.start()
    for c in here[:4]:
        c.wait()

    for q in range(2):
        wide = jnp.concatenate([ctab_ref[q], jnp.zeros((TILE - tiles, TILE), F32)], axis=0)
        tab_ref[q] = jnp.concatenate(three(jnp.transpose(wide)[:, :tiles]), axis=1)

    pairs = tiles * maxb
    flat = lax.broadcasted_iota(jnp.int32, (16, TILE), 0) * TILE + lax.broadcasted_iota(
        jnp.int32, (16, TILE), 1
    )
    lane = lax.broadcasted_iota(jnp.int32, (maxb, TILE), 1)
    sub = lax.broadcasted_iota(jnp.int32, (maxb, TILE), 0)

    def order(t, carry):
        lst, n0, n1, n2 = carry
        active = bc[t]
        lst = jnp.where(flat == 9 * TILE + t, active, lst)
        where_to = jnp.full((maxb, TILE), -1, jnp.int32)
        for k in range(maxb):
            p = t * maxb + k
            r = place(bl[k, t], me, odd, tiles)
            on = jnp.where(k < active, 1, 0)
            back = jnp.where(r >= 2 * tiles, on, 0)
            front = on - back
            at = jnp.where(on == 0, 2 * pairs + n2, jnp.where(back == 1, pairs + n1, n0))
            lst = jnp.where(flat == at, r * (2 * pairs) + p, lst)
            lst = jnp.where(flat == 3 * pairs + p, r, lst)
            n0, n1, n2 = n0 + front, n1 + back, n2 + 1 - on
            where_to = jnp.where(sub == k, r * on - (1 - on), where_to)
        oht_ref[pl.ds(pl.multiple_of(t * maxb, maxb), maxb), :] = jnp.where(
            lane == where_to, 1.0, 0.0
        )
        return lst, n0, n1, n2

    lst, n0, n1, n2 = lax.fori_loop(
        0, tiles, order, (jnp.full((16, TILE), pairs, jnp.int32), 0, 0, 0)
    )
    for c, count in enumerate((n0, n1, n2)):
        lst = jnp.where(flat == 8 * TILE + c, count, lst)
    lst_ref[...] = lst
    oh_ref[...] = jnp.transpose(oht_ref[...]).astype(jnp.bfloat16)

    low = lax.broadcasted_iota(jnp.int32, (TILE, TILE), 0)
    high = lax.broadcasted_iota(jnp.int32, (tiles, TILE), 0)

    low2 = jnp.concatenate([low, low], axis=1)
    high2 = jnp.concatenate([high, high], axis=1)

    def look_up(row, q, out, at):
        ids = jnp.concatenate([ids_ref[pl.ds(row + u, 1), :] for u in range(2)], axis=1)
        hit = jnp.where(high2 == lax.shift_right_logical(ids, 7), 1.0, 0.0).astype(jnp.bfloat16)
        got = jnp.dot(
            tab_ref[q], jnp.concatenate([hit, hit, hit], axis=0), preferred_element_type=F32
        )
        got = jnp.sum(jnp.where(low2 == (ids & 127), got, 0.0), axis=0, keepdims=True)
        for u in range(2):
            out[pl.ds(at + u, 1), :] = got[:, u * TILE : (u + 1) * TILE]

    here[4].wait()
    here[5].wait()

    def own_rows(i, _):
        for u in range(4):
            t = i * 8 + u * 2
            look_up(3 * tiles + t, 0, f0_ref, t)
            look_up(tiles + t, 1, g0_ref, tiles + t)
        return 0

    near[0].wait_recv()

    @pl.when(has_past)
    def _():
        onward.start()

    lax.fori_loop(0, tiles // 8, own_rows, 0)
    ft_ref[...] = jnp.transpose(
        jnp.concatenate([f0_ref[...], jnp.zeros((TILE - tiles, TILE), F32)], axis=0)
    )

    @pl.when(has_slow)
    def _():
        onward.wait_recv()

    @pl.when(jnp.logical_not(has_slow))
    def _():
        ids_ref[pl.ds(2 * tiles, tiles), :] = jnp.zeros((tiles, TILE), jnp.int32)

    def other_rows(i, _):
        for u in range(4):
            t = i * 8 + u * 2
            look_up(t, 1, g0_ref, t)
            look_up(2 * tiles + t, 1, g0_ref, 2 * tiles + t)
        return 0

    lax.fori_loop(0, tiles // 8, other_rows, 0)
    a0_ref[...] = jnp.exp2(g0_ref[...] * SCALE)
    here[6].wait()
    here[7].wait()
    near[1].wait_recv()
    near[0].wait_send()
    near[1].wait_send()

    @pl.when(has_past)
    def _():
        onward.wait_send()


def walk(
    which, pairs, maxb, tiles, lst, tile_of, x_ref, b0b_ref, k_ref, p1_ref, bufs
):
    def entry(i, u):
        at = which * pairs + i * WIDE + u
        v = lst[lax.shift_right_logical(at, 7), at & (TILE - 1)]
        p = v & (2 * pairs - 1)
        return p, lax.div(p, maxb), lax.div(v, 2 * pairs)

    def scores(i, u, buf):
        p, t, r = entry(i, u)
        buf[u] = lax.dot_general(
            x_ref[jnp.minimum(t, tiles - 1)], tile_of(r), NT, preferred_element_type=F32
        )

    def sums(i, u, buf):
        p, t, r = entry(i, u)
        kv = jnp.exp2(buf[u] * SCALE)
        k_ref[p] = kv
        p1_ref[pl.ds(p, 1), :] = jnp.sum(
            kv * b0b_ref[jnp.minimum(t, tiles - 1)], axis=0, keepdims=True
        )

    one, two = bufs

    def some(j, _):
        for u in range(WIDE):
            scores(2 * j + 1, u, two)
            sums(2 * j, u, one)
        for u in range(WIDE):
            scores(2 * j + 2, u, one)
            sums(2 * j + 1, u, two)
        return 0

    for u in range(WIDE):
        scores(0, u, one)
    lax.fori_loop(0, lax.div(lst[8, which] + 2 * WIDE - 1, 2 * WIDE), some, 0)


def kernel_n(
    tiles, maxb,
    lst, x_ref, of_ref, a0_ref, ft_ref, g0_ref, oh_ref,
    k_ref, p1_ref, f0b_ref, b0b_ref,
    one, two,
):
    pairs = tiles * maxb
    p1_ref[...] = jnp.zeros(p1_ref.shape, F32)
    lanes = lax.broadcasted_iota(jnp.int32, (TILE, TILE), 1)

    def spread(i, _):
        for u in range(4):
            t = i * 4 + u
            col = jnp.sum(jnp.where(lanes == t, ft_ref[...], 0.0), axis=1, keepdims=True)
            f0 = jnp.broadcast_to(col, (TILE, TILE))
            f0b_ref[t] = f0
            b0b_ref[t] = jnp.exp2(f0 * SCALE)
        return 0

    lax.fori_loop(0, tiles // 4, spread, 0)

    def absent(i, _):
        at = 2 * pairs + i
        k_ref[lst[lax.shift_right_logical(at, 7), at & (TILE - 1)] & (2 * pairs - 1)] = jnp.zeros(
            (TILE, TILE), F32
        )
        return 0

    lax.fori_loop(0, lst[8, 2], absent, 0)
    walk(
        0, pairs, maxb, tiles, lst, lambda r: of_ref[jnp.minimum(r, 2 * tiles - 1)],
        x_ref, b0b_ref, k_ref, p1_ref, (one, two),
    )


def fetch(r, ybuf, of_ref, es_ref, tiles):
    @pl.when(r < 2 * tiles)
    def _():
        ybuf[...] = of_ref[jnp.minimum(r, 2 * tiles - 1)]

    @pl.when(r >= 2 * tiles)
    def _():
        ybuf[...] = es_ref[jnp.clip(r - 2 * tiles, 0, tiles - 1)]


def kernel_b(
    tiles, maxb, log_size,
    lst, es_ref, k_in, p1_in, f0b_ref, b0b_ref, g0_ref, a0_ref, x_ref, of_ref, oh_ref,
    k_ref, p1_ref, f1b_ref, b1b_ref, c1_ref, c2_ref, bad_ref,
    ybuf, cols, one, two,
):
    pairs = tiles * maxb
    walk(
        1, pairs, maxb, tiles, lst, lambda r: es_ref[jnp.clip(r - 2 * tiles, 0, tiles - 1)],
        x_ref, b0b_ref, k_ref, p1_ref, (one, two),
    )

    def finish(i, worst):
        for u in range(4):
            t = i * 4 + u
            total = jnp.zeros((TILE, TILE), F32)
            for k in range(maxb):
                at = 3 * pairs + t * maxb + k
                r = jnp.clip(lst[lax.shift_right_logical(at, 7), at & (TILE - 1)], 0, 3 * tiles - 1)
                total = total + k_ref[t * maxb + k] * a0_ref[pl.ds(r, 1), :]
            total = jnp.sum(total, axis=1, keepdims=True)
            worst = jnp.maximum(worst, jnp.where((total >= LO) & (total <= HI), 0.0, 1.0))
            lse = jnp.broadcast_to(jnp.log(total), (TILE, TILE))
            f1 = 0.5 * (f0b_ref[t] + log_size - EPSILON * lse)
            f1b_ref[t] = f1
            b1b_ref[t] = jnp.exp2(f1 * SCALE)
        return worst

    worst = lax.fori_loop(0, tiles // 4, finish, jnp.zeros((TILE, 1), F32))
    onehot = oh_ref[...]
    here = jnp.sum(onehot.astype(F32), axis=1, keepdims=True) > 0.5
    total = add_up(onehot, p1_ref[:pairs])
    fits = (total >= LO) & (total <= HI)
    c1_ref[...] = jnp.where(here, jnp.log(total), NEGATIVE)[: 3 * tiles]
    wrong = jnp.where(here & jnp.logical_not(fits), 1.0, 0.0)
    bad = jnp.maximum(jnp.max(worst), jnp.max(wrong))
    bad_ref[...] = jnp.full((8, TILE), bad)
    c2_ref[...] = jnp.full((3 * tiles, TILE), NEGATIVE, F32)

    @pl.when(bad > 0.5)
    def _():
        for c in range(4):
            cols[c] = jnp.full((3 * tiles, TILE), NEGATIVE if c % 2 == 0 else 0.0, F32)

        def column(c, r, terms):
            top = cols[c, pl.ds(r, 1), :]
            now = jnp.maximum(top, jnp.max(terms, axis=0, keepdims=True))
            cols[c + 1, pl.ds(r, 1), :] = cols[c + 1, pl.ds(r, 1), :] * jnp.exp(top - now) + jnp.sum(
                jnp.exp(terms - now), axis=0, keepdims=True
            )
            cols[c, pl.ds(r, 1), :] = now

        def one(t, _):
            x = x_ref[t]
            f0 = f0b_ref[t]

            def slot(k, carry):
                top, total = carry
                at = 3 * pairs + t * maxb + k
                r = lst[lax.shift_right_logical(at, 7), at & (TILE - 1)]
                fetch(r, ybuf, of_ref, es_ref, tiles)
                s = lax.dot_general(x, ybuf[...], NT, preferred_element_type=F32)
                terms = (g0_ref[pl.ds(r, 1), :] + s) / EPSILON
                now = jnp.maximum(top, jnp.max(terms, axis=1, keepdims=True))
                total = total * jnp.exp(top - now) + jnp.sum(
                    jnp.exp(terms - now), axis=1, keepdims=True
                )
                column(0, r, (f0 + s) / EPSILON)
                return now, total

            count = lst[9, t]
            top, total = lax.fori_loop(
                0, count, slot, (jnp.full((TILE, 1), NEGATIVE, F32), jnp.zeros((TILE, 1), F32))
            )
            lse = jnp.broadcast_to(top + jnp.log(total), (TILE, TILE))
            f1b_ref[t] = 0.5 * (f0 + log_size - EPSILON * lse)

            def again(k, _):
                at = 3 * pairs + t * maxb + k
                r = lst[lax.shift_right_logical(at, 7), at & (TILE - 1)]
                fetch(r, ybuf, of_ref, es_ref, tiles)
                s = lax.dot_general(x, ybuf[...], NT, preferred_element_type=F32)
                column(2, r, (f1b_ref[t] + s) / EPSILON)
                return 0

            lax.fori_loop(0, count, again, 0)
            return 0

        lax.fori_loop(0, tiles, one, 0)
        c1_ref[...] = jnp.where(cols[1] > 0, cols[0] + jnp.log(cols[1]), NEGATIVE)
        c2_ref[...] = jnp.where(cols[3] > 0, cols[2] + jnp.log(cols[3]), NEGATIVE)


def merge(*parts):
    top = functools.reduce(jnp.maximum, parts)
    return top + jnp.log(functools.reduce(jnp.add, [jnp.exp(p - top) for p in parts]))


def kernel_f(
    n, tiles, maxb, log_size,
    lst_ref, k_ref, f1b_ref, b1b_ref, g0_ref, oh_ref, c1_ref, c2s_ref, bad_ref,
    f2_ref, g2_ref, g1_ref,
    lst, p2_ref, c2_ref, a1_ref, ft_ref, got_f, got_s, got_fs, got_sf, got2_f, got2_s,
    send, recv, local,
):
    me, odd, fast, slow, has_slow = partners(n)
    past_fast, past_slow = fast + 1 - 2 * odd, slow - 1 + 2 * odd
    has_past = (past_fast >= 0) & (past_fast < n)
    sems = (send, recv)
    pairs = tiles * maxb
    listing = pltpu.make_async_copy(lst_ref, lst, local)
    listing.start()
    greet(fast)

    @pl.when(has_slow)
    def _():
        greet(slow)
        greet(past_slow)

    @pl.when(has_past)
    def _():
        greet(past_fast)

    to_slow = remote(c1_ref.at[pl.ds(tiles, 2 * tiles)], got_s, sems, 0, slow)
    to_past_fast = remote(c1_ref.at[pl.ds(0, tiles)], got_sf, sems, 1, past_fast)
    to_past_slow = remote(c1_ref.at[pl.ds(2 * tiles, tiles)], got_fs, sems, 2, past_slow)
    to_fast = remote(c1_ref.at[pl.ds(0, 2 * tiles)], got_f, sems, 3, fast)
    pl.semaphore_wait(
        pltpu.get_barrier_semaphore(),
        1 + jnp.where(has_slow, 2, 0) + jnp.where(has_past, 1, 0),
    )

    @pl.when(has_past)
    def _():
        to_past_fast.start()

    @pl.when(has_slow)
    def _():
        to_past_slow.start()
        to_slow.start()

    to_fast.start()

    def columns(i, _):
        for u in range(2):
            t = i * 2 + u
            b1 = b1b_ref[t]
            p2_ref[pl.ds(pl.multiple_of(t * maxb, maxb), maxb), :] = jnp.concatenate(
                [jnp.sum(k_ref[t * maxb + k] * b1, axis=0, keepdims=True) for k in range(maxb)],
                axis=0,
            )
        return 0

    lax.fori_loop(0, tiles // 2, columns, 0)
    total = add_up(oh_ref[...], p2_ref[...])[: 3 * tiles]
    quick = jnp.where(total > 0, jnp.log(total), NEGATIVE)
    c2_ref[...] = jnp.where(bad_ref[0:1, :] > 0.5, c2s_ref[...], quick)

    to_fast.wait_recv()
    @pl.when(has_past)
    def _():
        to_past_slow.wait_recv()

    @pl.when(jnp.logical_not(has_past))
    def _():
        got_fs[...] = jnp.full((tiles, TILE), NEGATIVE, F32)

    @pl.when(has_slow)
    def _():
        to_past_fast.wait_recv()
        to_slow.wait_recv()

    @pl.when(jnp.logical_not(has_slow))
    def _():
        got_sf[...] = jnp.full((tiles, TILE), NEGATIVE, F32)
        got_s[:tiles] = jnp.zeros((tiles, TILE), F32)
        got_s[tiles:] = jnp.full((tiles, TILE), NEGATIVE, F32)
        got2_s[...] = jnp.full((tiles, TILE), NEGATIVE, F32)

    own = pl.ds(tiles, tiles)
    front, back = pl.ds(0, tiles), pl.ds(2 * tiles, tiles)
    for part, lse in (
        (front, merge(c1_ref[front, :], got_f[own, :], got_fs[...])),
        (own, merge(c1_ref[own, :], got_f[front, :], got_s[own, :])),
        (back, merge(c1_ref[back, :], got_s[front, :], got_sf[...])),
    ):
        g1 = 0.5 * (g0_ref[part, :] + log_size - EPSILON * lse)
        g1_ref[part, :] = g1
        a1_ref[part, :] = jnp.exp2(g1 * SCALE)
    last_slow = remote(c2_ref.at[back], got2_s, sems, 4, slow)
    last_fast = remote(c2_ref.at[front], got2_f, sems, 5, fast)

    @pl.when(has_slow)
    def _():
        last_slow.start()

    last_fast.start()
    listing.wait()
    lanes = lax.broadcasted_iota(jnp.int32, (TILE, TILE), 1)
    ft_ref[...] = jnp.zeros((TILE, TILE), F32)

    def rows(i, _):
        for u in range(4):
            t = i * 4 + u
            total = jnp.zeros((TILE, TILE), F32)
            for k in range(maxb):
                at = 3 * pairs + t * maxb + k
                r = jnp.clip(lst[lax.shift_right_logical(at, 7), at & (TILE - 1)], 0, 3 * tiles - 1)
                total = total + k_ref[t * maxb + k] * a1_ref[pl.ds(r, 1), :]
            total = jnp.sum(total, axis=1, keepdims=True)
            fits = (total >= LO) & (total <= HI)
            lse = jnp.broadcast_to(jnp.log(jnp.where(fits, total, jnp.nan)), (TILE, TILE))
            f2 = 0.5 * (f1b_ref[t] + log_size - EPSILON * lse)
            ft_ref[...] = jnp.where(lanes == t, f2, ft_ref[...])
        return 0

    lax.fori_loop(0, tiles // 4, rows, 0)
    f2_ref[...] = jnp.transpose(ft_ref[...])[:tiles]
    last_fast.wait_recv()

    @pl.when(has_slow)
    def _():
        last_slow.wait_recv()

    lse = merge(c2_ref[own, :], got2_f[...], got2_s[...])
    g2_ref[...] = 0.5 * (g1_ref[own, :] + log_size - EPSILON * lse)
    to_fast.wait_send()
    last_fast.wait_send()

    @pl.when(has_slow)
    def _():
        to_slow.wait_send()
        to_past_slow.wait_send()
        last_slow.wait_send()

    @pl.when(has_past)
    def _():
        to_past_fast.wait_send()


def kernel_g(
    tiles, maxb, log_size,
    lst_ref, f2_in, g2_in, g1_ref, bad_ref, f1b_ref, x_ref, of_ref, es_ref,
    f2_ref, g2_ref, lst, ft_ref, ybuf, sem,
):
    pairs = tiles * maxb
    f2 = f2_in[...]
    f2_ref[...] = f2
    g2_ref[...] = g2_in[...]
    bad = jnp.maximum(
        jnp.maximum(jnp.max(jnp.where(f2 == f2, 0.0, 1.0)), jnp.max(bad_ref[...])),
        jnp.max(jnp.where(jnp.abs(g1_ref[...]) <= FAR, 0.0, 1.0)),
    )

    @pl.when(bad > 0.5)
    def _():
        listing = pltpu.make_async_copy(lst_ref, lst, sem)
        listing.start()
        listing.wait()
        lanes = lax.broadcasted_iota(jnp.int32, (TILE, TILE), 1)
        ft_ref[...] = jnp.zeros((TILE, TILE), F32)

        def one(t, _):
            x = x_ref[t]

            def slot(k, carry):
                top, total = carry
                at = 3 * pairs + t * maxb + k
                r = lst[lax.shift_right_logical(at, 7), at & (TILE - 1)]
                fetch(r, ybuf, of_ref, es_ref, tiles)
                s = lax.dot_general(x, ybuf[...], NT, preferred_element_type=F32)
                terms = (g1_ref[pl.ds(r, 1), :] + s) / EPSILON
                now = jnp.maximum(top, jnp.max(terms, axis=1, keepdims=True))
                total = total * jnp.exp(top - now) + jnp.sum(
                    jnp.exp(terms - now), axis=1, keepdims=True
                )
                return now, total

            top, total = lax.fori_loop(
                0, lst[9, t], slot, (jnp.full((TILE, 1), NEGATIVE, F32), jnp.zeros((TILE, 1), F32))
            )
            lse = jnp.broadcast_to(top + jnp.log(total), (TILE, TILE))
            f2 = 0.5 * (f1b_ref[t] + log_size - EPSILON * lse)
            ft_ref[...] = jnp.where(lanes == t, f2, ft_ref[...])
            return 0

        lax.fori_loop(0, tiles, one, 0)
        f2_ref[...] = jnp.transpose(ft_ref[...])[:tiles]


def shards(n, src, tgt, scl, tcl, cs, ct, bl, bc):
    rows, width = src.shape
    tiles = rows // TILE
    maxb = bl.shape[1]
    pairs = tiles * maxb
    log_size = EPSILON * math.log(rows * n)
    bf = jnp.bfloat16
    cost = lambda flops: pl.CostEstimate(flops=flops, bytes_accessed=1 << 23, transcendentals=0)
    flops = 2 * pairs * TILE * TILE * width
    by_tile = lambda a: a.reshape(tiles, TILE, width)
    rows_of = lambda a: a.reshape(tiles, TILE)
    table = lambda a: a.reshape(a.shape[0] // TILE, TILE)
    block, line = (tiles, TILE, TILE), (3 * tiles, TILE)
    dma = pltpu.SemaphoreType.DMA
    route = [(i, i + 1) for i in range(1, n - 1, 2)]
    far = by_tile(lax.ppermute(tgt, "row", route + [(b, a) for a, b in route]))

    ft, g0, a0, x, of, oh, lst = pl.pallas_call(
        functools.partial(kernel_a, n, tiles, maxb),
        out_shape=(
            VM((TILE, TILE), F32),
            VM(line, F32),
            VM(line, F32),
            VM((tiles, TILE, width), bf),
            VM((2 * tiles, TILE, width), bf),
            VM((TILE, pairs), bf),
            VM((16, TILE), jnp.int32),
        ),
        in_specs=[FAR_MEM] * 8,
        out_specs=(SPEC,) * 7,
        scratch_shapes=[
            pltpu.SMEM((maxb, tiles), jnp.int32),
            pltpu.SMEM((tiles,), jnp.int32),
            VM((4 * tiles, TILE), jnp.int32),
            VM((2, tiles, TILE), F32),
            VM((2, TILE, 3 * tiles), bf),
            VM((tiles, TILE), F32),
            VM((pairs, TILE), F32),
            dma((3,)),
            dma((3,)),
            dma((8,)),
        ],
        compiler_params=pltpu.CompilerParams(
            collective_id=0, has_side_effects=True, vmem_limit_bytes=WHOLE
        ),
        cost_estimate=cost(flops),
        name="exchange",
    )(bl.T, bc, by_tile(src), by_tile(tgt), rows_of(scl), rows_of(tcl), table(cs), table(ct))

    steps = [VM((WIDE, TILE, TILE), F32)] * 2
    sums = (
        VM((pairs + 1, TILE, TILE), F32),
        VM((pairs + 8, TILE), F32),
    )
    k, p1, f0b, b0b = pl.pallas_call(
        functools.partial(kernel_n, tiles, maxb),
        out_shape=sums + (VM(block, F32),) * 2,
        in_specs=[SMEM] + [SPEC] * 6,
        out_specs=(SPEC,) * 4,
        scratch_shapes=steps,
        compiler_params=pltpu.CompilerParams(vmem_limit_bytes=LIMIT),
        cost_estimate=cost(flops),
        name="near_pairs",
    )(lst, x, of, a0, ft, g0, oh)

    k, p1, f1b, b1b, c1, c2s, bad = pl.pallas_call(
        functools.partial(kernel_b, tiles, maxb, log_size),
        out_shape=sums
        + (
            VM(block, F32),
            VM(block, F32),
            VM(line, F32),
            VM(line, F32),
            VM((8, TILE), F32),
        ),
        in_specs=[SMEM] + [SPEC] * 10,
        out_specs=(SPEC,) * 7,
        scratch_shapes=[VM((TILE, width), bf), VM((4,) + line, F32)] + steps,
        input_output_aliases={2: 0, 3: 1},
        compiler_params=pltpu.CompilerParams(vmem_limit_bytes=LIMIT),
        cost_estimate=cost(flops),
        name="far_pairs",
    )(lst, far, k, p1, f0b, b0b, g0, a0, x, of, oh)

    f2, g2, g1 = pl.pallas_call(
        functools.partial(kernel_f, n, tiles, maxb, log_size),
        out_shape=(VM((tiles, TILE), F32), VM((tiles, TILE), F32), VM(line, F32)),
        in_specs=[ANY] + [SPEC] * 8,
        out_specs=(SPEC,) * 3,
        scratch_shapes=[
            pltpu.SMEM((16, TILE), jnp.int32),
            VM((pairs, TILE), F32),
            VM(line, F32),
            VM(line, F32),
            VM((TILE, TILE), F32),
            VM((2 * tiles, TILE), F32),
            VM((2 * tiles, TILE), F32),
            VM((tiles, TILE), F32),
            VM((tiles, TILE), F32),
            VM((tiles, TILE), F32),
            VM((tiles, TILE), F32),
            dma((6,)),
            dma((6,)),
            dma,
        ],
        compiler_params=pltpu.CompilerParams(
            collective_id=1, has_side_effects=True, vmem_limit_bytes=LIMIT
        ),
        cost_estimate=cost(flops),
        name="potentials",
    )(lst, k, f1b, b1b, g0, oh, c1, c2s, bad)

    f2, g2 = pl.pallas_call(
        functools.partial(kernel_g, tiles, maxb, log_size),
        out_shape=(jax.ShapeDtypeStruct((tiles, TILE), F32),) * 2,
        in_specs=[ANY] + [SPEC] * 8,
        out_specs=(SPEC,) * 2,
        scratch_shapes=[
            pltpu.SMEM((16, TILE), jnp.int32),
            VM((TILE, TILE), F32),
            VM((TILE, width), bf),
            dma,
        ],
        compiler_params=pltpu.CompilerParams(vmem_limit_bytes=LIMIT),
        cost_estimate=cost(flops),
        name="guard",
    )(lst, f2, g2, g1, bad, f1b, x, of, far)
    return f2.reshape(rows), g2.reshape(rows)


LIMIT = 5 << 20
WHOLE = 48 << 20


def solution(mesh):
    both = P(("grp", "row"))
    wide = P(("grp", "row"), None)
    return jax.shard_map(
        functools.partial(shards, mesh.shape["row"]),
        mesh=mesh,
        in_specs=(wide, wide, both, both, P("grp"), P("grp"), wide, both),
        out_specs=(both, both),
        check_vma=False,
    )
```

```python
import functools
import math

import jax
import jax.numpy as jnp
from jax import lax
from jax.experimental import pallas as pl
from jax.experimental.pallas import tpu as pltpu
from jax.sharding import PartitionSpec as P

TILE = 128
ITERS = 2
EPSILON = 0.5
NEGATIVE = -1e30
SCALE = 1.0 / (EPSILON * math.log(2.0))
MESH = pl.DeviceIdType.MESH
VM = pltpu.VMEM
F32 = jnp.float32
SPEC = pl.BlockSpec(memory_space=pltpu.VMEM)
SMEM = pl.BlockSpec(memory_space=pltpu.SMEM)
ANY = pl.BlockSpec(memory_space=pl.ANY)
FAR_MEM = pl.BlockSpec(memory_space=pltpu.HBM)
NT = (((1,), (1,)), ((), ()))
LO, HI = 1e-8, 1e20
FAR = 15.0


def partners(n):
    me = lax.axis_index("row")
    odd = lax.rem(me, 2)
    slow = me - 1 + 2 * odd
    return me, odd, me + 1 - 2 * odd, slow, (slow >= 0) & (slow < n)


def place(listed, me, odd, tiles):
    w = listed - (me - 1) * tiles
    turned = jnp.where(w >= 2 * tiles, w - 2 * tiles, jnp.where(w < tiles, w + 2 * tiles, w))
    return jnp.where(odd == 1, w, turned)


def greet(device):
    pl.semaphore_signal(
        pltpu.get_barrier_semaphore(), inc=1, device_id={"row": device}, device_id_type=MESH
    )


def remote(src, dst, sems, i, device):
    send, recv = sems
    return pltpu.make_async_remote_copy(
        src_ref=src,
        dst_ref=dst,
        send_sem=send.at[i],
        recv_sem=recv.at[i],
        device_id={"row": device},
        device_id_type=MESH,
    )


def three(x):
    a = x.astype(jnp.bfloat16)
    rest = x - a.astype(F32)
    b = rest.astype(jnp.bfloat16)
    c = (rest - b.astype(F32)).astype(jnp.bfloat16)
    return a, b, c


def add_up(onehot, parts):
    a, b, c = three(parts)
    dot = lambda y: jnp.dot(onehot, y, preferred_element_type=F32)
    return dot(a) + (dot(b) + dot(c))


def kernel_a(
    n, tiles, maxb,
    bl_hbm, bc_hbm, src, tgt, scl, tcl, cs_hbm, ct_hbm,
    g0_ref, x_ref, of_ref, oh_ref, lst_ref,
    bl, bc, ids_ref, ctab_ref, tab_ref, oht_ref, send, recv, local,
):
    me, odd, fast, slow, has_slow = partners(n)
    sems = (send, recv)
    here = [
        pltpu.make_async_copy(bl_hbm, bl, local.at[0]),
        pltpu.make_async_copy(bc_hbm, bc, local.at[1]),
        pltpu.make_async_copy(cs_hbm, ctab_ref.at[0], local.at[2]),
        pltpu.make_async_copy(ct_hbm, ctab_ref.at[1], local.at[3]),
        pltpu.make_async_copy(tcl, ids_ref.at[pl.ds(tiles, tiles)], local.at[4]),
        pltpu.make_async_copy(scl, ids_ref.at[pl.ds(3 * tiles, tiles)], local.at[5]),
        pltpu.make_async_copy(tgt, of_ref.at[pl.ds(tiles, tiles)], local.at[6]),
        pltpu.make_async_copy(src, x_ref, local.at[7]),
    ]
    past_fast, past_slow = fast + 1 - 2 * odd, slow - 1 + 2 * odd
    has_past = (past_fast >= 0) & (past_fast < n)
    greet(fast)

    @pl.when(has_slow)
    def _():
        greet(past_slow)

    for c in here:
        c.start()
    pl.semaphore_wait(pltpu.get_barrier_semaphore(), 1 + jnp.where(has_past, 1, 0))
    near = [
        remote(tcl, ids_ref.at[pl.ds(0, tiles)], sems, 0, fast),
        remote(tgt, of_ref.at[pl.ds(0, tiles)], sems, 1, fast),
    ]
    onward = remote(
        ids_ref.at[pl.ds(0, tiles)], ids_ref.at[pl.ds(2 * tiles, tiles)], sems, 2, past_fast
    )
    for c in near:
        c.start()
    for c in here[:4]:
        c.wait()

    for q in range(2):
        wide = jnp.concatenate([ctab_ref[q], jnp.zeros((TILE - tiles, TILE), F32)], axis=0)
        tab_ref[q] = jnp.concatenate(three(jnp.transpose(wide)[:, :tiles]), axis=1)

    pairs = tiles * maxb
    flat = lax.broadcasted_iota(jnp.int32, (16, TILE), 0) * TILE + lax.broadcasted_iota(
        jnp.int32, (16, TILE), 1
    )
    lane = lax.broadcasted_iota(jnp.int32, (maxb, TILE), 1)
    sub = lax.broadcasted_iota(jnp.int32, (maxb, TILE), 0)

    def order(t, carry):
        lst, n0, n1, n2 = carry
        active = bc[t]
        lst = jnp.where(flat == 9 * TILE + t, active, lst)
        where_to = jnp.full((maxb, TILE), -1, jnp.int32)
        for k in range(maxb):
            p = t * maxb + k
            r = place(bl[k, t], me, odd, tiles)
            on = jnp.where(k < active, 1, 0)
            back = jnp.where(r >= 2 * tiles, on, 0)
            front = on - back
            at = jnp.where(on == 0, 2 * pairs + n2, jnp.where(back == 1, pairs + n1, n0))
            entry = (r - 2 * tiles * back) * (1 << 20) + t * (1 << 12) + p
            lst = jnp.where(flat == at, entry, lst)
            lst = jnp.where(flat == 3 * pairs + p, r, lst)
            n0, n1, n2 = n0 + front, n1 + back, n2 + 1 - on
            where_to = jnp.where(sub == k, r * on - (1 - on), where_to)
        oht_ref[pl.ds(pl.multiple_of(t * maxb, maxb), maxb), :] = jnp.where(
            lane == where_to, 1.0, 0.0
        )
        return lst, n0, n1, n2

    lst, n0, n1, n2 = lax.fori_loop(
        0, tiles, order, (jnp.full((16, TILE), tiles * (1 << 12) + pairs, jnp.int32), 0, 0, 0)
    )
    for c, count in enumerate((n0, n1, n2)):
        lst = jnp.where(flat == 8 * TILE + c, count, lst)
    lst_ref[...] = lst
    oh_ref[...] = jnp.transpose(oht_ref[...]).astype(jnp.bfloat16)

    low = lax.broadcasted_iota(jnp.int32, (TILE, TILE), 0)
    high = lax.broadcasted_iota(jnp.int32, (tiles, TILE), 0)

    low2 = jnp.concatenate([low, low], axis=1)
    high2 = jnp.concatenate([high, high], axis=1)

    def look_up(row, q, out, at):
        ids = jnp.concatenate([ids_ref[pl.ds(row + u, 1), :] for u in range(2)], axis=1)
        hit = jnp.where(high2 == lax.shift_right_logical(ids, 7), 1.0, 0.0).astype(jnp.bfloat16)
        got = jnp.dot(
            tab_ref[q], jnp.concatenate([hit, hit, hit], axis=0), preferred_element_type=F32
        )
        got = jnp.sum(jnp.where(low2 == (ids & 127), got, 0.0), axis=0, keepdims=True)
        for u in range(2):
            out[pl.ds(at + u, 1), :] = got[:, u * TILE : (u + 1) * TILE]

    here[4].wait()
    here[5].wait()

    def own_rows(i, _):
        for u in range(4):
            t = i * 8 + u * 2
            look_up(3 * tiles + t, 0, g0_ref, 3 * tiles + t)
            look_up(tiles + t, 1, g0_ref, tiles + t)
        return 0

    near[0].wait_recv()

    @pl.when(has_past)
    def _():
        onward.start()

    lax.fori_loop(0, tiles // 8, own_rows, 0)

    @pl.when(has_slow)
    def _():
        onward.wait_recv()

    @pl.when(jnp.logical_not(has_slow))
    def _():
        ids_ref[pl.ds(2 * tiles, tiles), :] = jnp.zeros((tiles, TILE), jnp.int32)

    def other_rows(i, _):
        for u in range(4):
            t = i * 8 + u * 2
            look_up(t, 1, g0_ref, t)
            look_up(2 * tiles + t, 1, g0_ref, 2 * tiles + t)
        return 0

    lax.fori_loop(0, tiles // 8, other_rows, 0)
    g0_ref[4 * tiles :] = jnp.exp2(g0_ref[: 3 * tiles] * SCALE)
    here[6].wait()
    here[7].wait()
    near[1].wait_recv()
    near[0].wait_send()
    near[1].wait_send()

    @pl.when(has_past)
    def _():
        onward.wait_send()


def walk(which, wide, pairs, lst, y_ref, shift, x_ref, a0_ref, b0b_ref, k_ref, ra_ref, p1_ref):
    line = TILE // wide

    def some(i, _):
        row = which * (pairs // TILE) + lax.div(i, line)
        col = lax.rem(i, line) * wide
        for u in range(wide):
            v = lst[row, col + u]
            p = v & ((1 << 12) - 1)
            t = lax.shift_right_logical(v, 12) & 255
            r = lax.shift_right_logical(v, 20)
            real = jnp.minimum(t, x_ref.shape[0] - 1)
            s = lax.dot_general(x_ref[real], y_ref[r], NT, preferred_element_type=F32)
            kv = jnp.exp2(s * SCALE)
            k_ref[p] = kv
            ra_ref[t] = ra_ref[t] + kv * a0_ref[pl.ds(r + shift, 1), :]
            p1_ref[pl.ds(p, 1), :] = jnp.sum(kv * b0b_ref[real], axis=0, keepdims=True)
        return 0

    lax.fori_loop(0, lax.div(lst[8, which] + wide - 1, wide), some, 0)


def kernel_n(
    tiles, maxb,
    lst, x_ref, of_ref, g0_ref, oh_ref,
    k_ref, ra_ref, p1_ref, f0b_ref, b0b_ref,
):
    pairs = tiles * maxb
    p1_ref[...] = jnp.zeros(p1_ref.shape, F32)
    turned = jnp.transpose(
        jnp.concatenate([g0_ref[3 * tiles : 4 * tiles], jnp.zeros((TILE - tiles, TILE), F32)], axis=0)
    )
    for t in range(tiles):
        f0 = jnp.broadcast_to(turned[:, t : t + 1], (TILE, TILE))
        f0b_ref[t] = f0
        b0b_ref[t] = jnp.exp2(f0 * SCALE)
        ra_ref[t] = jnp.zeros((TILE, TILE), F32)

    def absent(i, _):
        at = 2 * pairs + i
        k_ref[lst[lax.shift_right_logical(at, 7), at & (TILE - 1)] & 4095] = jnp.zeros(
            (TILE, TILE), F32
        )
        return 0

    lax.fori_loop(0, lst[8, 2], absent, 0)
    walk(0, 32, pairs, lst, of_ref, 4 * tiles, x_ref, g0_ref, b0b_ref, k_ref, ra_ref, p1_ref)


def fetch(r, ybuf, of_ref, es_ref, tiles):
    @pl.when(r < 2 * tiles)
    def _():
        ybuf[...] = of_ref[jnp.minimum(r, 2 * tiles - 1)]

    @pl.when(r >= 2 * tiles)
    def _():
        ybuf[...] = es_ref[jnp.clip(r - 2 * tiles, 0, tiles - 1)]


def kernel_b(
    tiles, maxb, log_size,
    lst, es_ref, k_in, ra_in, p1_in, f0b_ref, b0b_ref, g0_ref, x_ref, of_ref, oh_ref,
    k_ref, ra_ref, p1_ref, f1b_ref, b1b_ref, c1_ref, c2_ref, bad_ref,
    ybuf, cols,
):
    pairs = tiles * maxb
    walk(
        1, 16, pairs, lst, es_ref, 6 * tiles, x_ref, g0_ref, b0b_ref, k_ref, ra_ref, p1_ref
    )

    def finish(i, worst):
        for u in range(8):
            t = i * 8 + u
            total = jnp.sum(ra_ref[t], axis=1, keepdims=True)
            worst = jnp.maximum(worst, jnp.where((total >= LO) & (total <= HI), 0.0, 1.0))
            lse = jnp.broadcast_to(jnp.log(total), (TILE, TILE))
            f1 = 0.5 * (f0b_ref[t] + log_size - EPSILON * lse)
            f1b_ref[t] = f1
            b1b_ref[t] = jnp.exp2(f1 * SCALE)
        return worst

    worst = lax.fori_loop(0, tiles // 8, finish, jnp.zeros((TILE, 1), F32))
    onehot = oh_ref[...]
    here = jnp.sum(onehot.astype(F32), axis=1, keepdims=True) > 0.5
    total = add_up(onehot, p1_ref[:pairs])
    fits = (total >= LO) & (total <= HI)
    c1_ref[...] = jnp.where(here, jnp.log(total), NEGATIVE)[: 3 * tiles]
    wrong = jnp.where(here & jnp.logical_not(fits), 1.0, 0.0)
    bad = jnp.maximum(jnp.max(worst), jnp.max(wrong))
    bad_ref[...] = jnp.full((8, TILE), bad)
    c2_ref[...] = jnp.full((3 * tiles, TILE), NEGATIVE, F32)

    @pl.when(bad > 0.5)
    def _():
        for c in range(4):
            cols[c] = jnp.full((3 * tiles, TILE), NEGATIVE if c % 2 == 0 else 0.0, F32)

        def column(c, r, terms):
            top = cols[c, pl.ds(r, 1), :]
            now = jnp.maximum(top, jnp.max(terms, axis=0, keepdims=True))
            cols[c + 1, pl.ds(r, 1), :] = cols[c + 1, pl.ds(r, 1), :] * jnp.exp(top - now) + jnp.sum(
                jnp.exp(terms - now), axis=0, keepdims=True
            )
            cols[c, pl.ds(r, 1), :] = now

        def one(t, _):
            x = x_ref[t]
            f0 = f0b_ref[t]

            def slot(k, carry):
                top, total = carry
                at = 3 * pairs + t * maxb + k
                r = lst[lax.shift_right_logical(at, 7), at & (TILE - 1)]
                fetch(r, ybuf, of_ref, es_ref, tiles)
                s = lax.dot_general(x, ybuf[...], NT, preferred_element_type=F32)
                terms = (g0_ref[pl.ds(r, 1), :] + s) / EPSILON
                now = jnp.maximum(top, jnp.max(terms, axis=1, keepdims=True))
                total = total * jnp.exp(top - now) + jnp.sum(
                    jnp.exp(terms - now), axis=1, keepdims=True
                )
                column(0, r, (f0 + s) / EPSILON)
                return now, total

            count = lst[9, t]
            top, total = lax.fori_loop(
                0, count, slot, (jnp.full((TILE, 1), NEGATIVE, F32), jnp.zeros((TILE, 1), F32))
            )
            lse = jnp.broadcast_to(top + jnp.log(total), (TILE, TILE))
            f1b_ref[t] = 0.5 * (f0 + log_size - EPSILON * lse)

            def again(k, _):
                at = 3 * pairs + t * maxb + k
                r = lst[lax.shift_right_logical(at, 7), at & (TILE - 1)]
                fetch(r, ybuf, of_ref, es_ref, tiles)
                s = lax.dot_general(x, ybuf[...], NT, preferred_element_type=F32)
                column(2, r, (f1b_ref[t] + s) / EPSILON)
                return 0

            lax.fori_loop(0, count, again, 0)
            return 0

        lax.fori_loop(0, tiles, one, 0)
        c1_ref[...] = jnp.where(cols[1] > 0, cols[0] + jnp.log(cols[1]), NEGATIVE)
        c2_ref[...] = jnp.where(cols[3] > 0, cols[2] + jnp.log(cols[3]), NEGATIVE)


def merge(*parts):
    top = functools.reduce(jnp.maximum, parts)
    return top + jnp.log(functools.reduce(jnp.add, [jnp.exp(p - top) for p in parts]))


def kernel_f(
    n, tiles, maxb, log_size,
    lst_ref, k_ref, f1b_ref, b1b_ref, g0_ref, oh_ref, c1_ref, c2s_ref, bad_ref,
    f2_ref, g2_ref, g1_ref,
    lst, p2_ref, c2_ref, a1_ref, ft_ref, got_f, got_s, got_fs, got_sf, got2_f, got2_s,
    send, recv, local,
):
    me, odd, fast, slow, has_slow = partners(n)
    past_fast, past_slow = fast + 1 - 2 * odd, slow - 1 + 2 * odd
    has_past = (past_fast >= 0) & (past_fast < n)
    sems = (send, recv)
    pairs = tiles * maxb
    listing = pltpu.make_async_copy(lst_ref, lst, local)
    listing.start()
    greet(fast)

    @pl.when(has_slow)
    def _():
        greet(slow)
        greet(past_slow)

    @pl.when(has_past)
    def _():
        greet(past_fast)

    to_slow = remote(c1_ref.at[pl.ds(tiles, 2 * tiles)], got_s, sems, 0, slow)
    to_past_fast = remote(c1_ref.at[pl.ds(0, tiles)], got_sf, sems, 1, past_fast)
    to_past_slow = remote(c1_ref.at[pl.ds(2 * tiles, tiles)], got_fs, sems, 2, past_slow)
    to_fast = remote(c1_ref.at[pl.ds(0, 2 * tiles)], got_f, sems, 3, fast)
    pl.semaphore_wait(
        pltpu.get_barrier_semaphore(),
        1 + jnp.where(has_slow, 2, 0) + jnp.where(has_past, 1, 0),
    )

    @pl.when(has_past)
    def _():
        to_past_fast.start()

    @pl.when(has_slow)
    def _():
        to_past_slow.start()
        to_slow.start()

    to_fast.start()

    def columns(i, _):
        for u in range(2):
            t = i * 2 + u
            b1 = b1b_ref[t]
            p2_ref[pl.ds(pl.multiple_of(t * maxb, maxb), maxb), :] = jnp.concatenate(
                [jnp.sum(k_ref[t * maxb + k] * b1, axis=0, keepdims=True) for k in range(maxb)],
                axis=0,
            )
        return 0

    lax.fori_loop(0, tiles // 2, columns, 0)
    total = add_up(oh_ref[...], p2_ref[...])[: 3 * tiles]
    quick = jnp.where(total > 0, jnp.log(total), NEGATIVE)
    c2_ref[...] = jnp.where(bad_ref[0:1, :] > 0.5, c2s_ref[...], quick)

    to_fast.wait_recv()
    @pl.when(has_past)
    def _():
        to_past_slow.wait_recv()

    @pl.when(jnp.logical_not(has_past))
    def _():
        got_fs[...] = jnp.full((tiles, TILE), NEGATIVE, F32)

    @pl.when(has_slow)
    def _():
        to_past_fast.wait_recv()
        to_slow.wait_recv()

    @pl.when(jnp.logical_not(has_slow))
    def _():
        got_sf[...] = jnp.full((tiles, TILE), NEGATIVE, F32)
        got_s[:tiles] = jnp.zeros((tiles, TILE), F32)
        got_s[tiles:] = jnp.full((tiles, TILE), NEGATIVE, F32)
        got2_s[...] = jnp.full((tiles, TILE), NEGATIVE, F32)

    own = pl.ds(tiles, tiles)
    front, back = pl.ds(0, tiles), pl.ds(2 * tiles, tiles)
    for part, lse in (
        (front, merge(c1_ref[front, :], got_f[own, :], got_fs[...])),
        (own, merge(c1_ref[own, :], got_f[front, :], got_s[own, :])),
        (back, merge(c1_ref[back, :], got_s[front, :], got_sf[...])),
    ):
        g1 = 0.5 * (g0_ref[part, :] + log_size - EPSILON * lse)
        g1_ref[part, :] = g1
        a1_ref[part, :] = jnp.exp2(g1 * SCALE)
    last_slow = remote(c2_ref.at[back], got2_s, sems, 4, slow)
    last_fast = remote(c2_ref.at[front], got2_f, sems, 5, fast)

    @pl.when(has_slow)
    def _():
        last_slow.start()

    last_fast.start()
    listing.wait()
    lanes = lax.broadcasted_iota(jnp.int32, (TILE, TILE), 1)
    ft_ref[...] = jnp.zeros((TILE, TILE), F32)

    def rows(i, _):
        for u in range(4):
            t = i * 4 + u
            total = jnp.zeros((TILE, TILE), F32)
            for k in range(maxb):
                at = 3 * pairs + t * maxb + k
                r = jnp.clip(lst[lax.shift_right_logical(at, 7), at & (TILE - 1)], 0, 3 * tiles - 1)
                total = total + k_ref[t * maxb + k] * a1_ref[pl.ds(r, 1), :]
            total = jnp.sum(total, axis=1, keepdims=True)
            fits = (total >= LO) & (total <= HI)
            lse = jnp.broadcast_to(jnp.log(jnp.where(fits, total, jnp.nan)), (TILE, TILE))
            f2 = 0.5 * (f1b_ref[t] + log_size - EPSILON * lse)
            ft_ref[...] = jnp.where(lanes == t, f2, ft_ref[...])
        return 0

    lax.fori_loop(0, tiles // 4, rows, 0)
    f2_ref[...] = jnp.transpose(ft_ref[...])[:tiles]
    last_fast.wait_recv()

    @pl.when(has_slow)
    def _():
        last_slow.wait_recv()

    lse = merge(c2_ref[own, :], got2_f[...], got2_s[...])
    g2_ref[...] = 0.5 * (g1_ref[own, :] + log_size - EPSILON * lse)
    to_fast.wait_send()
    last_fast.wait_send()

    @pl.when(has_slow)
    def _():
        to_slow.wait_send()
        to_past_slow.wait_send()
        last_slow.wait_send()

    @pl.when(has_past)
    def _():
        to_past_fast.wait_send()


def kernel_g(
    tiles, maxb, log_size,
    lst_ref, f2_in, g2_in, g1_ref, bad_ref, f1b_ref, x_ref, of_ref, es_ref,
    f2_ref, g2_ref, lst, ft_ref, ybuf, sem,
):
    pairs = tiles * maxb
    f2 = f2_in[...]
    f2_ref[...] = f2
    g2_ref[...] = g2_in[...]
    bad = jnp.maximum(
        jnp.maximum(jnp.max(jnp.where(f2 == f2, 0.0, 1.0)), jnp.max(bad_ref[...])),
        jnp.max(jnp.where(jnp.abs(g1_ref[...]) <= FAR, 0.0, 1.0)),
    )

    @pl.when(bad > 0.5)
    def _():
        listing = pltpu.make_async_copy(lst_ref, lst, sem)
        listing.start()
        listing.wait()
        lanes = lax.broadcasted_iota(jnp.int32, (TILE, TILE), 1)
        ft_ref[...] = jnp.zeros((TILE, TILE), F32)

        def one(t, _):
            x = x_ref[t]

            def slot(k, carry):
                top, total = carry
                at = 3 * pairs + t * maxb + k
                r = lst[lax.shift_right_logical(at, 7), at & (TILE - 1)]
                fetch(r, ybuf, of_ref, es_ref, tiles)
                s = lax.dot_general(x, ybuf[...], NT, preferred_element_type=F32)
                terms = (g1_ref[pl.ds(r, 1), :] + s) / EPSILON
                now = jnp.maximum(top, jnp.max(terms, axis=1, keepdims=True))
                total = total * jnp.exp(top - now) + jnp.sum(
                    jnp.exp(terms - now), axis=1, keepdims=True
                )
                return now, total

            top, total = lax.fori_loop(
                0, lst[9, t], slot, (jnp.full((TILE, 1), NEGATIVE, F32), jnp.zeros((TILE, 1), F32))
            )
            lse = jnp.broadcast_to(top + jnp.log(total), (TILE, TILE))
            f2 = 0.5 * (f1b_ref[t] + log_size - EPSILON * lse)
            ft_ref[...] = jnp.where(lanes == t, f2, ft_ref[...])
            return 0

        lax.fori_loop(0, tiles, one, 0)
        f2_ref[...] = jnp.transpose(ft_ref[...])[:tiles]


def shards(n, src, tgt, scl, tcl, cs, ct, bl, bc):
    rows, width = src.shape
    tiles = rows // TILE
    maxb = bl.shape[1]
    pairs = tiles * maxb
    log_size = EPSILON * math.log(rows * n)
    bf = jnp.bfloat16
    cost = lambda flops: pl.CostEstimate(flops=flops, bytes_accessed=1 << 23, transcendentals=0)
    flops = 2 * pairs * TILE * TILE * width
    by_tile = lambda a: a.reshape(tiles, TILE, width)
    rows_of = lambda a: a.reshape(tiles, TILE)
    table = lambda a: a.reshape(a.shape[0] // TILE, TILE)
    block, line = (tiles, TILE, TILE), (3 * tiles, TILE)
    dma = pltpu.SemaphoreType.DMA
    route = [(i, i + 1) for i in range(1, n - 1, 2)]
    far = by_tile(lax.ppermute(tgt, "row", route + [(b, a) for a, b in route]))

    g0, x, of, oh, lst = pl.pallas_call(
        functools.partial(kernel_a, n, tiles, maxb),
        out_shape=(
            VM((7 * tiles, TILE), F32),
            VM((tiles, TILE, width), bf),
            VM((2 * tiles, TILE, width), bf),
            VM((TILE, pairs), bf),
            VM((16, TILE), jnp.int32),
        ),
        in_specs=[FAR_MEM] * 8,
        out_specs=(SPEC,) * 5,
        scratch_shapes=[
            pltpu.SMEM((maxb, tiles), jnp.int32),
            pltpu.SMEM((tiles,), jnp.int32),
            VM((4 * tiles, TILE), jnp.int32),
            VM((2, tiles, TILE), F32),
            VM((2, TILE, 3 * tiles), bf),
            VM((pairs, TILE), F32),
            dma((3,)),
            dma((3,)),
            dma((8,)),
        ],
        compiler_params=pltpu.CompilerParams(
            collective_id=0, has_side_effects=True, vmem_limit_bytes=WHOLE
        ),
        cost_estimate=cost(flops),
        name="exchange",
    )(bl.T, bc, by_tile(src), by_tile(tgt), rows_of(scl), rows_of(tcl), table(cs), table(ct))

    sums = (
        VM((pairs + 1, TILE, TILE), F32),
        VM((tiles + 1, TILE, TILE), F32),
        VM((pairs + 8, TILE), F32),
    )
    k, ra, p1, f0b, b0b = pl.pallas_call(
        functools.partial(kernel_n, tiles, maxb),
        out_shape=sums + (VM(block, F32),) * 2,
        in_specs=[SMEM] + [SPEC] * 4,
        out_specs=(SPEC,) * 5,
        compiler_params=pltpu.CompilerParams(vmem_limit_bytes=LIMIT),
        cost_estimate=cost(flops),
        name="near_pairs",
    )(lst, x, of, g0, oh)

    k, ra, p1, f1b, b1b, c1, c2s, bad = pl.pallas_call(
        functools.partial(kernel_b, tiles, maxb, log_size),
        out_shape=sums
        + (
            VM(block, F32),
            VM(block, F32),
            VM(line, F32),
            VM(line, F32),
            VM((8, TILE), F32),
        ),
        in_specs=[SMEM] + [SPEC] * 10,
        out_specs=(SPEC,) * 8,
        scratch_shapes=[VM((TILE, width), bf), VM((4,) + line, F32)],
        input_output_aliases={2: 0, 3: 1, 4: 2},
        compiler_params=pltpu.CompilerParams(vmem_limit_bytes=LIMIT),
        cost_estimate=cost(flops),
        name="far_pairs",
    )(lst, far, k, ra, p1, f0b, b0b, g0, x, of, oh)

    f2, g2, g1 = pl.pallas_call(
        functools.partial(kernel_f, n, tiles, maxb, log_size),
        out_shape=(VM((tiles, TILE), F32), VM((tiles, TILE), F32), VM(line, F32)),
        in_specs=[ANY] + [SPEC] * 8,
        out_specs=(SPEC,) * 3,
        scratch_shapes=[
            pltpu.SMEM((16, TILE), jnp.int32),
            VM((pairs, TILE), F32),
            VM(line, F32),
            VM(line, F32),
            VM((TILE, TILE), F32),
            VM((2 * tiles, TILE), F32),
            VM((2 * tiles, TILE), F32),
            VM((tiles, TILE), F32),
            VM((tiles, TILE), F32),
            VM((tiles, TILE), F32),
            VM((tiles, TILE), F32),
            dma((6,)),
            dma((6,)),
            dma,
        ],
        compiler_params=pltpu.CompilerParams(
            collective_id=1, has_side_effects=True, vmem_limit_bytes=LIMIT
        ),
        cost_estimate=cost(flops),
        name="potentials",
    )(lst, k, f1b, b1b, g0, oh, c1, c2s, bad)

    f2, g2 = pl.pallas_call(
        functools.partial(kernel_g, tiles, maxb, log_size),
        out_shape=(jax.ShapeDtypeStruct((tiles, TILE), F32),) * 2,
        in_specs=[ANY] + [SPEC] * 8,
        out_specs=(SPEC,) * 2,
        scratch_shapes=[
            pltpu.SMEM((16, TILE), jnp.int32),
            VM((TILE, TILE), F32),
            VM((TILE, width), bf),
            dma,
        ],
        compiler_params=pltpu.CompilerParams(vmem_limit_bytes=LIMIT),
        cost_estimate=cost(flops),
        name="guard",
    )(lst, f2, g2, g1, bad, f1b, x, of, far)
    return f2.reshape(rows), g2.reshape(rows)


LIMIT = 5 << 20
WHOLE = 49664 << 10


def solution(mesh):
    both = P(("grp", "row"))
    wide = P(("grp", "row"), None)
    return jax.shard_map(
        functools.partial(shards, mesh.shape["row"]),
        mesh=mesh,
        in_specs=(wide, wide, both, both, P("grp"), P("grp"), wide, both),
        out_specs=(both, both),
        check_vma=False,
    )
```

```python
import functools
import math

import jax
import jax.numpy as jnp
from jax import lax
from jax.experimental import pallas as pl
from jax.experimental.pallas import tpu as pltpu
from jax.sharding import PartitionSpec as P

TILE = 128
ITERS = 2
EPSILON = 0.5
NEGATIVE = -1e30
SCALE = 1.0 / (EPSILON * math.log(2.0))
MESH = pl.DeviceIdType.MESH
VM = pltpu.VMEM
F32 = jnp.float32
SPEC = pl.BlockSpec(memory_space=pltpu.VMEM)
SMEM = pl.BlockSpec(memory_space=pltpu.SMEM)
ANY = pl.BlockSpec(memory_space=pl.ANY)
FAR_MEM = pl.BlockSpec(memory_space=pltpu.HBM)
NT = (((1,), (1,)), ((), ()))
LO, HI = 1e-8, 1e20
FAR = 15.0


def partners(n):
    me = lax.axis_index("row")
    odd = lax.rem(me, 2)
    slow = me - 1 + 2 * odd
    return me, odd, me + 1 - 2 * odd, slow, (slow >= 0) & (slow < n)


def place(listed, me, odd, tiles):
    w = listed - (me - 1) * tiles
    turned = jnp.where(w >= 2 * tiles, w - 2 * tiles, jnp.where(w < tiles, w + 2 * tiles, w))
    return jnp.where(odd == 1, w, turned)


def greet(device):
    pl.semaphore_signal(
        pltpu.get_barrier_semaphore(), inc=1, device_id={"row": device}, device_id_type=MESH
    )


def remote(src, dst, sems, i, device):
    send, recv = sems
    return pltpu.make_async_remote_copy(
        src_ref=src,
        dst_ref=dst,
        send_sem=send.at[i],
        recv_sem=recv.at[i],
        device_id={"row": device},
        device_id_type=MESH,
    )


def three(x):
    a = x.astype(jnp.bfloat16)
    rest = x - a.astype(F32)
    b = rest.astype(jnp.bfloat16)
    c = (rest - b.astype(F32)).astype(jnp.bfloat16)
    return a, b, c


def add_up(onehot, parts):
    a, b, c = three(parts)
    dot = lambda y: jnp.dot(onehot, y, preferred_element_type=F32)
    return dot(a) + (dot(b) + dot(c))


def kernel_a(
    n, tiles, maxb,
    bl_hbm, bc_hbm, src, tgt, scl, tcl, cs_hbm, ct_hbm,
    g0_ref, x_ref, of_ref, oh_ref, lst_ref,
    bl, bc, ids_ref, ctab_ref, tab_ref, oht_ref, send, recv, local,
):
    me, odd, fast, slow, has_slow = partners(n)
    sems = (send, recv)
    here = [
        pltpu.make_async_copy(bl_hbm, bl, local.at[0]),
        pltpu.make_async_copy(bc_hbm, bc, local.at[1]),
        pltpu.make_async_copy(cs_hbm, ctab_ref.at[0], local.at[2]),
        pltpu.make_async_copy(ct_hbm, ctab_ref.at[1], local.at[3]),
        pltpu.make_async_copy(tcl, ids_ref.at[pl.ds(tiles, tiles)], local.at[4]),
        pltpu.make_async_copy(scl, ids_ref.at[pl.ds(3 * tiles, tiles)], local.at[5]),
        pltpu.make_async_copy(tgt, of_ref.at[pl.ds(tiles, tiles)], local.at[6]),
        pltpu.make_async_copy(src, x_ref, local.at[7]),
    ]
    past_fast, past_slow = fast + 1 - 2 * odd, slow - 1 + 2 * odd
    has_past = (past_fast >= 0) & (past_fast < n)
    greet(fast)

    @pl.when(has_slow)
    def _():
        greet(past_slow)

    for c in here:
        c.start()
    pl.semaphore_wait(pltpu.get_barrier_semaphore(), 1 + jnp.where(has_past, 1, 0))
    near = [
        remote(tcl, ids_ref.at[pl.ds(0, tiles)], sems, 0, fast),
        remote(tgt, of_ref.at[pl.ds(0, tiles)], sems, 1, fast),
    ]
    onward = remote(
        ids_ref.at[pl.ds(0, tiles)], ids_ref.at[pl.ds(2 * tiles, tiles)], sems, 2, past_fast
    )
    for c in near:
        c.start()
    for c in here[:4]:
        c.wait()

    for q in range(2):
        wide = jnp.concatenate([ctab_ref[q], jnp.zeros((TILE - tiles, TILE), F32)], axis=0)
        tab_ref[q] = jnp.concatenate(three(jnp.transpose(wide)[:, :tiles]), axis=1)

    pairs = tiles * maxb
    flat = lax.broadcasted_iota(jnp.int32, (16, TILE), 0) * TILE + lax.broadcasted_iota(
        jnp.int32, (16, TILE), 1
    )
    lane = lax.broadcasted_iota(jnp.int32, (maxb, TILE), 1)
    sub = lax.broadcasted_iota(jnp.int32, (maxb, TILE), 0)

    def order(t, carry):
        lst, n0, n1, n2 = carry
        active = bc[t]
        lst = jnp.where(flat == 9 * TILE + t, active, lst)
        where_to = jnp.full((maxb, TILE), -1, jnp.int32)
        for k in range(maxb):
            p = t * maxb + k
            r = place(bl[k, t], me, odd, tiles)
            on = jnp.where(k < active, 1, 0)
            back = jnp.where(r >= 2 * tiles, on, 0)
            front = on - back
            at = jnp.where(on == 0, 2 * pairs + n2, jnp.where(back == 1, pairs + n1, n0))
            entry = (r - 2 * tiles * back) * (1 << 20) + t * (1 << 12) + p
            lst = jnp.where(flat == at, entry, lst)
            lst = jnp.where(flat == 3 * pairs + p, r, lst)
            n0, n1, n2 = n0 + front, n1 + back, n2 + 1 - on
            where_to = jnp.where(sub == k, r * on - (1 - on), where_to)
        oht_ref[pl.ds(pl.multiple_of(t * maxb, maxb), maxb), :] = jnp.where(
            lane == where_to, 1.0, 0.0
        )
        return lst, n0, n1, n2

    lst, n0, n1, n2 = lax.fori_loop(
        0, tiles, order, (jnp.full((16, TILE), tiles * (1 << 12) + pairs, jnp.int32), 0, 0, 0)
    )
    for c, count in enumerate((n0, n1, n2)):
        lst = jnp.where(flat == 8 * TILE + c, count, lst)
    lst_ref[...] = lst
    oh_ref[...] = jnp.transpose(oht_ref[...]).astype(jnp.bfloat16)

    low = lax.broadcasted_iota(jnp.int32, (TILE, TILE), 0)
    high = lax.broadcasted_iota(jnp.int32, (tiles, TILE), 0)

    low2 = jnp.concatenate([low, low], axis=1)
    high2 = jnp.concatenate([high, high], axis=1)

    def look_up(row, q, out, at):
        ids = jnp.concatenate([ids_ref[pl.ds(row + u, 1), :] for u in range(2)], axis=1)
        hit = jnp.where(high2 == lax.shift_right_logical(ids, 7), 1.0, 0.0).astype(jnp.bfloat16)
        got = jnp.dot(
            tab_ref[q], jnp.concatenate([hit, hit, hit], axis=0), preferred_element_type=F32
        )
        got = jnp.sum(jnp.where(low2 == (ids & 127), got, 0.0), axis=0, keepdims=True)
        for u in range(2):
            out[pl.ds(at + u, 1), :] = got[:, u * TILE : (u + 1) * TILE]

    here[4].wait()
    here[5].wait()

    def own_rows(i, _):
        for u in range(4):
            t = i * 8 + u * 2
            look_up(3 * tiles + t, 0, g0_ref, 3 * tiles + t)
            look_up(tiles + t, 1, g0_ref, tiles + t)
        return 0

    near[0].wait_recv()

    @pl.when(has_past)
    def _():
        onward.start()

    lax.fori_loop(0, tiles // 8, own_rows, 0)

    @pl.when(has_slow)
    def _():
        onward.wait_recv()

    @pl.when(jnp.logical_not(has_slow))
    def _():
        ids_ref[pl.ds(2 * tiles, tiles), :] = jnp.zeros((tiles, TILE), jnp.int32)

    def other_rows(i, _):
        for u in range(4):
            t = i * 8 + u * 2
            look_up(t, 1, g0_ref, t)
            look_up(2 * tiles + t, 1, g0_ref, 2 * tiles + t)
        return 0

    lax.fori_loop(0, tiles // 8, other_rows, 0)
    g0_ref[4 * tiles :] = jnp.exp2(g0_ref[: 3 * tiles] * SCALE)
    here[6].wait()
    here[7].wait()
    near[1].wait_recv()
    near[0].wait_send()
    near[1].wait_send()

    @pl.when(has_past)
    def _():
        onward.wait_send()


def walk(which, wide, pairs, lst, y_ref, shift, x_ref, a0_ref, b0b_ref, k_ref, ra_ref, p1_ref):
    line = TILE // wide

    def some(i, _):
        row = which * (pairs // TILE) + lax.div(i, line)
        col = lax.rem(i, line) * wide
        for u in range(wide):
            v = lst[row, col + u]
            p = v & ((1 << 12) - 1)
            t = lax.shift_right_logical(v, 12) & 255
            r = lax.shift_right_logical(v, 20)
            real = jnp.minimum(t, x_ref.shape[0] - 1)
            s = lax.dot_general(x_ref[real], y_ref[r], NT, preferred_element_type=F32)
            kv = jnp.exp2(s * SCALE)
            k_ref[p] = kv
            ra_ref[t] = ra_ref[t] + kv * a0_ref[pl.ds(r + shift, 1), :]
            p1_ref[pl.ds(p, 1), :] = jnp.sum(kv * b0b_ref[real], axis=0, keepdims=True)
        return 0

    lax.fori_loop(0, lax.div(lst[8, which] + wide - 1, wide), some, 0)


def kernel_n(
    tiles, maxb,
    lst, x_ref, of_ref, g0_ref, oh_ref,
    k_ref, ra_ref, p1_ref, f0b_ref, b0b_ref,
):
    pairs = tiles * maxb
    p1_ref[...] = jnp.zeros(p1_ref.shape, F32)
    turned = jnp.transpose(
        jnp.concatenate([g0_ref[3 * tiles : 4 * tiles], jnp.zeros((TILE - tiles, TILE), F32)], axis=0)
    )
    for t in range(tiles):
        f0 = jnp.broadcast_to(turned[:, t : t + 1], (TILE, TILE))
        f0b_ref[t] = f0
        b0b_ref[t] = jnp.exp2(f0 * SCALE)
        ra_ref[t] = jnp.zeros((TILE, TILE), F32)

    def absent(i, _):
        at = 2 * pairs + i
        k_ref[lst[lax.shift_right_logical(at, 7), at & (TILE - 1)] & 4095] = jnp.zeros(
            (TILE, TILE), F32
        )
        return 0

    lax.fori_loop(0, lst[8, 2], absent, 0)
    walk(0, 32, pairs, lst, of_ref, 4 * tiles, x_ref, g0_ref, b0b_ref, k_ref, ra_ref, p1_ref)


def fetch(r, ybuf, of_ref, es_ref, tiles):
    @pl.when(r < 2 * tiles)
    def _():
        ybuf[...] = of_ref[jnp.minimum(r, 2 * tiles - 1)]

    @pl.when(r >= 2 * tiles)
    def _():
        ybuf[...] = es_ref[jnp.clip(r - 2 * tiles, 0, tiles - 1)]


def kernel_b(
    tiles, maxb, log_size,
    lst, es_ref, k_in, ra_in, p1_in, f0b_ref, b0b_ref, g0_ref, x_ref, of_ref, oh_ref,
    k_ref, ra_ref, p1_ref, f1b_ref, b1b_ref, c1_ref, c2_ref, bad_ref,
    ybuf, cols,
):
    pairs = tiles * maxb
    walk(
        1, 16, pairs, lst, es_ref, 6 * tiles, x_ref, g0_ref, b0b_ref, k_ref, ra_ref, p1_ref
    )

    def finish(i, worst):
        for u in range(8):
            t = i * 8 + u
            total = jnp.sum(ra_ref[t], axis=1, keepdims=True)
            worst = jnp.maximum(worst, jnp.where((total >= LO) & (total <= HI), 0.0, 1.0))
            lse = jnp.broadcast_to(jnp.log(total), (TILE, TILE))
            f1 = 0.5 * (f0b_ref[t] + log_size - EPSILON * lse)
            f1b_ref[t] = f1
            b1b_ref[t] = jnp.exp2(f1 * SCALE)
        return worst

    worst = lax.fori_loop(0, tiles // 8, finish, jnp.zeros((TILE, 1), F32))
    onehot = oh_ref[...]
    here = jnp.sum(onehot.astype(F32), axis=1, keepdims=True) > 0.5
    total = add_up(onehot, p1_ref[:pairs])
    fits = (total >= LO) & (total <= HI)
    c1_ref[...] = jnp.where(here, jnp.log(total), NEGATIVE)[: 3 * tiles]
    wrong = jnp.where(here & jnp.logical_not(fits), 1.0, 0.0)
    bad = jnp.maximum(jnp.max(worst), jnp.max(wrong))
    bad_ref[...] = jnp.full((8, TILE), bad)
    c2_ref[...] = jnp.full((3 * tiles, TILE), NEGATIVE, F32)

    @pl.when(bad > 0.5)
    def _():
        for c in range(4):
            cols[c] = jnp.full((3 * tiles, TILE), NEGATIVE if c % 2 == 0 else 0.0, F32)

        def column(c, r, terms):
            top = cols[c, pl.ds(r, 1), :]
            now = jnp.maximum(top, jnp.max(terms, axis=0, keepdims=True))
            cols[c + 1, pl.ds(r, 1), :] = cols[c + 1, pl.ds(r, 1), :] * jnp.exp(top - now) + jnp.sum(
                jnp.exp(terms - now), axis=0, keepdims=True
            )
            cols[c, pl.ds(r, 1), :] = now

        def one(t, _):
            x = x_ref[t]
            f0 = f0b_ref[t]

            def slot(k, carry):
                top, total = carry
                at = 3 * pairs + t * maxb + k
                r = lst[lax.shift_right_logical(at, 7), at & (TILE - 1)]
                fetch(r, ybuf, of_ref, es_ref, tiles)
                s = lax.dot_general(x, ybuf[...], NT, preferred_element_type=F32)
                terms = (g0_ref[pl.ds(r, 1), :] + s) / EPSILON
                now = jnp.maximum(top, jnp.max(terms, axis=1, keepdims=True))
                total = total * jnp.exp(top - now) + jnp.sum(
                    jnp.exp(terms - now), axis=1, keepdims=True
                )
                column(0, r, (f0 + s) / EPSILON)
                return now, total

            count = lst[9, t]
            top, total = lax.fori_loop(
                0, count, slot, (jnp.full((TILE, 1), NEGATIVE, F32), jnp.zeros((TILE, 1), F32))
            )
            lse = jnp.broadcast_to(top + jnp.log(total), (TILE, TILE))
            f1b_ref[t] = 0.5 * (f0 + log_size - EPSILON * lse)

            def again(k, _):
                at = 3 * pairs + t * maxb + k
                r = lst[lax.shift_right_logical(at, 7), at & (TILE - 1)]
                fetch(r, ybuf, of_ref, es_ref, tiles)
                s = lax.dot_general(x, ybuf[...], NT, preferred_element_type=F32)
                column(2, r, (f1b_ref[t] + s) / EPSILON)
                return 0

            lax.fori_loop(0, count, again, 0)
            return 0

        lax.fori_loop(0, tiles, one, 0)
        c1_ref[...] = jnp.where(cols[1] > 0, cols[0] + jnp.log(cols[1]), NEGATIVE)
        c2_ref[...] = jnp.where(cols[3] > 0, cols[2] + jnp.log(cols[3]), NEGATIVE)


def merge(*parts):
    top = functools.reduce(jnp.maximum, parts)
    return top + jnp.log(functools.reduce(jnp.add, [jnp.exp(p - top) for p in parts]))


def kernel_f(
    n, tiles, maxb, log_size,
    lst_ref, k_ref, f1b_ref, b1b_ref, g0_ref, oh_ref, c1_ref, c2s_ref, bad_ref,
    f2_ref, g2_ref, g1_ref,
    lst, p2_ref, c2_ref, a1_ref, ft_ref, got_f, got_s, got_fs, got_sf, got2_f, got2_s,
    send, recv, local,
):
    me, odd, fast, slow, has_slow = partners(n)
    past_fast, past_slow = fast + 1 - 2 * odd, slow - 1 + 2 * odd
    has_past = (past_fast >= 0) & (past_fast < n)
    sems = (send, recv)
    pairs = tiles * maxb
    listing = pltpu.make_async_copy(lst_ref, lst, local)
    listing.start()
    greet(fast)

    @pl.when(has_slow)
    def _():
        greet(slow)
        greet(past_slow)

    @pl.when(has_past)
    def _():
        greet(past_fast)

    to_slow = remote(c1_ref.at[pl.ds(tiles, 2 * tiles)], got_s, sems, 0, slow)
    to_past_fast = remote(c1_ref.at[pl.ds(0, tiles)], got_sf, sems, 1, past_fast)
    to_past_slow = remote(c1_ref.at[pl.ds(2 * tiles, tiles)], got_fs, sems, 2, past_slow)
    to_fast = remote(c1_ref.at[pl.ds(0, 2 * tiles)], got_f, sems, 3, fast)
    pl.semaphore_wait(
        pltpu.get_barrier_semaphore(),
        1 + jnp.where(has_slow, 2, 0) + jnp.where(has_past, 1, 0),
    )

    @pl.when(has_past)
    def _():
        to_past_fast.start()

    @pl.when(has_slow)
    def _():
        to_past_slow.start()
        to_slow.start()

    to_fast.start()

    def columns(i, _):
        for u in range(4):
            t = i * 4 + u
            b1 = b1b_ref[t]
            p2_ref[pl.ds(pl.multiple_of(t * maxb, maxb), maxb), :] = jnp.concatenate(
                [jnp.sum(k_ref[t * maxb + k] * b1, axis=0, keepdims=True) for k in range(maxb)],
                axis=0,
            )
        return 0

    lax.fori_loop(0, tiles // 4, columns, 0)
    total = add_up(oh_ref[...], p2_ref[...])[: 3 * tiles]
    quick = jnp.where(total > 0, jnp.log(total), NEGATIVE)
    c2_ref[...] = jnp.where(bad_ref[0:1, :] > 0.5, c2s_ref[...], quick)

    own = pl.ds(tiles, tiles)
    front, back = pl.ds(0, tiles), pl.ds(2 * tiles, tiles)
    last_slow = remote(c2_ref.at[back], got2_s, sems, 4, slow)
    last_fast = remote(c2_ref.at[front], got2_f, sems, 5, fast)
    listing.wait()
    to_fast.wait_recv()

    @pl.when(has_slow)
    def _():
        last_slow.start()

    last_fast.start()

    @pl.when(has_past)
    def _():
        to_past_slow.wait_recv()

    @pl.when(jnp.logical_not(has_past))
    def _():
        got_fs[...] = jnp.full((tiles, TILE), NEGATIVE, F32)

    @pl.when(has_slow)
    def _():
        to_past_fast.wait_recv()
        to_slow.wait_recv()

    @pl.when(jnp.logical_not(has_slow))
    def _():
        got_sf[...] = jnp.full((tiles, TILE), NEGATIVE, F32)
        got_s[:tiles] = jnp.zeros((tiles, TILE), F32)
        got_s[tiles:] = jnp.full((tiles, TILE), NEGATIVE, F32)
        got2_s[...] = jnp.full((tiles, TILE), NEGATIVE, F32)

    for part, lse in (
        (front, merge(c1_ref[front, :], got_f[own, :], got_fs[...])),
        (own, merge(c1_ref[own, :], got_f[front, :], got_s[own, :])),
        (back, merge(c1_ref[back, :], got_s[front, :], got_sf[...])),
    ):
        g1 = 0.5 * (g0_ref[part, :] + log_size - EPSILON * lse)
        g1_ref[part, :] = g1
        a1_ref[part, :] = jnp.exp2(g1 * SCALE)
    lanes = lax.broadcasted_iota(jnp.int32, (TILE, TILE), 1)
    ft_ref[...] = jnp.zeros((TILE, TILE), F32)

    def rows(i, _):
        turned = ft_ref[...]
        for u in range(8):
            t = i * 8 + u
            total = jnp.zeros((TILE, TILE), F32)
            for k in range(maxb):
                at = 3 * pairs + t * maxb + k
                r = jnp.clip(lst[lax.shift_right_logical(at, 7), at & (TILE - 1)], 0, 3 * tiles - 1)
                total = total + k_ref[t * maxb + k] * a1_ref[pl.ds(r, 1), :]
            total = jnp.sum(total, axis=1, keepdims=True)
            fits = (total >= LO) & (total <= HI)
            lse = jnp.broadcast_to(jnp.log(jnp.where(fits, total, jnp.nan)), (TILE, TILE))
            f2 = 0.5 * (f1b_ref[t] + log_size - EPSILON * lse)
            turned = jnp.where(lanes == t, f2, turned)
        ft_ref[...] = turned
        return 0

    lax.fori_loop(0, tiles // 8, rows, 0)
    f2_ref[...] = jnp.transpose(ft_ref[...])[:tiles]
    last_fast.wait_recv()

    @pl.when(has_slow)
    def _():
        last_slow.wait_recv()

    lse = merge(c2_ref[own, :], got2_f[...], got2_s[...])
    g2_ref[...] = 0.5 * (g1_ref[own, :] + log_size - EPSILON * lse)
    to_fast.wait_send()
    last_fast.wait_send()

    @pl.when(has_slow)
    def _():
        to_slow.wait_send()
        to_past_slow.wait_send()
        last_slow.wait_send()

    @pl.when(has_past)
    def _():
        to_past_fast.wait_send()


def kernel_g(
    tiles, maxb, log_size,
    lst_ref, f2_in, g2_in, g1_ref, bad_ref, f1b_ref, x_ref, of_ref, es_ref,
    f2_ref, g2_ref, lst, ft_ref, ybuf, sem,
):
    pairs = tiles * maxb
    f2 = f2_in[...]
    f2_ref[...] = f2
    g2_ref[...] = g2_in[...]
    bad = jnp.maximum(
        jnp.maximum(jnp.max(jnp.where(f2 == f2, 0.0, 1.0)), jnp.max(bad_ref[...])),
        jnp.max(jnp.where(jnp.abs(g1_ref[...]) <= FAR, 0.0, 1.0)),
    )

    @pl.when(bad > 0.5)
    def _():
        listing = pltpu.make_async_copy(lst_ref, lst, sem)
        listing.start()
        listing.wait()
        lanes = lax.broadcasted_iota(jnp.int32, (TILE, TILE), 1)
        ft_ref[...] = jnp.zeros((TILE, TILE), F32)

        def one(t, _):
            x = x_ref[t]

            def slot(k, carry):
                top, total = carry
                at = 3 * pairs + t * maxb + k
                r = lst[lax.shift_right_logical(at, 7), at & (TILE - 1)]
                fetch(r, ybuf, of_ref, es_ref, tiles)
                s = lax.dot_general(x, ybuf[...], NT, preferred_element_type=F32)
                terms = (g1_ref[pl.ds(r, 1), :] + s) / EPSILON
                now = jnp.maximum(top, jnp.max(terms, axis=1, keepdims=True))
                total = total * jnp.exp(top - now) + jnp.sum(
                    jnp.exp(terms - now), axis=1, keepdims=True
                )
                return now, total

            top, total = lax.fori_loop(
                0, lst[9, t], slot, (jnp.full((TILE, 1), NEGATIVE, F32), jnp.zeros((TILE, 1), F32))
            )
            lse = jnp.broadcast_to(top + jnp.log(total), (TILE, TILE))
            f2 = 0.5 * (f1b_ref[t] + log_size - EPSILON * lse)
            ft_ref[...] = jnp.where(lanes == t, f2, ft_ref[...])
            return 0

        lax.fori_loop(0, tiles, one, 0)
        f2_ref[...] = jnp.transpose(ft_ref[...])[:tiles]


def shards(n, src, tgt, scl, tcl, cs, ct, bl, bc):
    rows, width = src.shape
    tiles = rows // TILE
    maxb = bl.shape[1]
    pairs = tiles * maxb
    log_size = EPSILON * math.log(rows * n)
    bf = jnp.bfloat16
    cost = lambda flops: pl.CostEstimate(flops=flops, bytes_accessed=1 << 23, transcendentals=0)
    flops = 2 * pairs * TILE * TILE * width
    by_tile = lambda a: a.reshape(tiles, TILE, width)
    rows_of = lambda a: a.reshape(tiles, TILE)
    table = lambda a: a.reshape(a.shape[0] // TILE, TILE)
    block, line = (tiles, TILE, TILE), (3 * tiles, TILE)
    dma = pltpu.SemaphoreType.DMA
    route = [(i, i + 1) for i in range(1, n - 1, 2)]
    far = by_tile(lax.ppermute(tgt, "row", route + [(b, a) for a, b in route]))

    g0, x, of, oh, lst = pl.pallas_call(
        functools.partial(kernel_a, n, tiles, maxb),
        out_shape=(
            VM((7 * tiles, TILE), F32),
            VM((tiles, TILE, width), bf),
            VM((2 * tiles, TILE, width), bf),
            VM((TILE, pairs), bf),
            VM((16, TILE), jnp.int32),
        ),
        in_specs=[FAR_MEM] * 8,
        out_specs=(SPEC,) * 5,
        scratch_shapes=[
            pltpu.SMEM((maxb, tiles), jnp.int32),
            pltpu.SMEM((tiles,), jnp.int32),
            VM((4 * tiles, TILE), jnp.int32),
            VM((2, tiles, TILE), F32),
            VM((2, TILE, 3 * tiles), bf),
            VM((pairs, TILE), F32),
            dma((3,)),
            dma((3,)),
            dma((8,)),
        ],
        compiler_params=pltpu.CompilerParams(
            collective_id=0, has_side_effects=True, vmem_limit_bytes=WHOLE
        ),
        cost_estimate=cost(flops),
        name="exchange",
    )(bl.T, bc, by_tile(src), by_tile(tgt), rows_of(scl), rows_of(tcl), table(cs), table(ct))

    sums = (
        VM((pairs + 1, TILE, TILE), F32),
        VM((tiles + 1, TILE, TILE), F32),
        VM((pairs + 8, TILE), F32),
    )
    k, ra, p1, f0b, b0b = pl.pallas_call(
        functools.partial(kernel_n, tiles, maxb),
        out_shape=sums + (VM(block, F32),) * 2,
        in_specs=[SMEM] + [SPEC] * 4,
        out_specs=(SPEC,) * 5,
        compiler_params=pltpu.CompilerParams(vmem_limit_bytes=LIMIT),
        cost_estimate=cost(flops),
        name="near_pairs",
    )(lst, x, of, g0, oh)

    k, ra, p1, f1b, b1b, c1, c2s, bad = pl.pallas_call(
        functools.partial(kernel_b, tiles, maxb, log_size),
        out_shape=sums
        + (
            VM(block, F32),
            VM(block, F32),
            VM(line, F32),
            VM(line, F32),
            VM((8, TILE), F32),
        ),
        in_specs=[SMEM] + [SPEC] * 10,
        out_specs=(SPEC,) * 8,
        scratch_shapes=[VM((TILE, width), bf), VM((4,) + line, F32)],
        input_output_aliases={2: 0, 3: 1, 4: 2},
        compiler_params=pltpu.CompilerParams(vmem_limit_bytes=LIMIT),
        cost_estimate=cost(flops),
        name="far_pairs",
    )(lst, far, k, ra, p1, f0b, b0b, g0, x, of, oh)

    f2, g2, g1 = pl.pallas_call(
        functools.partial(kernel_f, n, tiles, maxb, log_size),
        out_shape=(VM((tiles, TILE), F32), VM((tiles, TILE), F32), VM(line, F32)),
        in_specs=[ANY] + [SPEC] * 8,
        out_specs=(SPEC,) * 3,
        scratch_shapes=[
            pltpu.SMEM((16, TILE), jnp.int32),
            VM((pairs, TILE), F32),
            VM(line, F32),
            VM(line, F32),
            VM((TILE, TILE), F32),
            VM((2 * tiles, TILE), F32),
            VM((2 * tiles, TILE), F32),
            VM((tiles, TILE), F32),
            VM((tiles, TILE), F32),
            VM((tiles, TILE), F32),
            VM((tiles, TILE), F32),
            dma((6,)),
            dma((6,)),
            dma,
        ],
        compiler_params=pltpu.CompilerParams(
            collective_id=1, has_side_effects=True, vmem_limit_bytes=LIMIT
        ),
        cost_estimate=cost(flops),
        name="potentials",
    )(lst, k, f1b, b1b, g0, oh, c1, c2s, bad)

    f2, g2 = pl.pallas_call(
        functools.partial(kernel_g, tiles, maxb, log_size),
        out_shape=(jax.ShapeDtypeStruct((tiles, TILE), F32),) * 2,
        in_specs=[ANY] + [SPEC] * 8,
        out_specs=(SPEC,) * 2,
        scratch_shapes=[
            pltpu.SMEM((16, TILE), jnp.int32),
            VM((TILE, TILE), F32),
            VM((TILE, width), bf),
            dma,
        ],
        compiler_params=pltpu.CompilerParams(vmem_limit_bytes=LIMIT),
        cost_estimate=cost(flops),
        name="guard",
    )(lst, f2, g2, g1, bad, f1b, x, of, far)
    return f2.reshape(rows), g2.reshape(rows)


LIMIT = 5 << 20
WHOLE = 49664 << 10


def solution(mesh):
    both = P(("grp", "row"))
    wide = P(("grp", "row"), None)
    return jax.shard_map(
        functools.partial(shards, mesh.shape["row"]),
        mesh=mesh,
        in_specs=(wide, wide, both, both, P("grp"), P("grp"), wide, both),
        out_specs=(both, both),
        check_vma=False,
    )
```
